256 devices in a mesh: dp: 32 (over y, x, core), section: 8 (over z).
Axes of the slice: x: 4, y: 4, z: 8, core: 2. Of those that a mesh axis runs over, the one named last changes fastest.
Arguments:
- activations: bfloat16 [4, 2048, 2048], P(None, 'dp'), may hold values from -6 to 6
- cotangent: bfloat16 [4, 2048, 2048], P(None, 'dp'), may hold values from -6 to 6
- weight: bfloat16 [8, 2048, 2048], P('section', 'dp'), may hold values from -0.125 to 0.125
- norm_gain: float32 [8, 2048], P('section'), may hold values from 0.1 to 1.9
- pair_mask: int32 [8, 512, 2048], P('section'), may hold values from 0 to 5, as said below
- earlier_mask: int32 [8, 512, 2048], P('section', 'dp'), may hold values from 0 to 5, as said below
Outputs:
- weight_grad: float32 [8, 2048, 2048], P('section', 'dp')
- flip_count: int32 [8], P('section')
The draws below stay inside these ranges and needn't reach their ends.
Inputs may be any that keep to these rules, and one draw needn't show every extreme that they name: `pair_mask`: pair number of each group of four consecutive rows and each column; pairs numbered (0,1), (0,2), (0,3), (1,2), (1,3), (2,3). `earlier_mask`: pair numbers of the previous step, numbered likewise.
All inputs are finite; a program needn't handle non-finite values.
Results may differ from the reference program's by a relative error of at most 0.02.
Values may be sent and summed in bfloat16 or wider, within the bound.
No kernel may reach another device: no remote copies, remote signals or barrier semaphores. Data moves between devices by JAX's collectives and lax.ppermute only.
A program may use at most 64 MiB of HBM per device.

```python
import math
import jax
import jax.numpy as jnp
from jax import lax

D = 2048
MICRO = 4
SECTIONS = 8
BATCH_ROWS = 2048
TOKENS = 8192
N_DP = 32


def mask_pair(key):
    base_key = jax.random.fold_in(key, 7301)
    mask_shape = (SECTIONS, D // 4, D)
    current = jax.random.randint(jax.random.fold_in(base_key, 1), mask_shape, 0, 6)
    row_iota = lax.broadcasted_iota(jnp.int32, mask_shape, 1)
    threshold = 100 + 200 * row_iota // (D // 4 - 1)
    dice_rolls = jax.random.randint(jax.random.fold_in(base_key, 2), mask_shape, 0, 1000)
    offsets = jax.random.randint(jax.random.fold_in(base_key, 3), mask_shape, 1, 6)
    earlier = jnp.where(dice_rolls < threshold, (current + offsets) % 6, current)
    return (current.astype(jnp.int32), earlier.astype(jnp.int32))


def draw_pair_mask(key, part):
    return mask_pair(key)[0]


def draw_earlier_mask(key, part):
    return mask_pair(key)[1]


def levels(rng, shape, cuts, smallest, high):
    gain, own = 1.0, jax.random.fold_in(rng, 6)
    for position, blocks in cuts:
        steps = jnp.exp(jax.random.uniform(jax.random.fold_in(own, position), (blocks,), jnp.float32, smallest / len(cuts), high / len(cuts)))
        gain = gain * jnp.repeat(steps, shape[position] // blocks).reshape([-1 if axis == position else 1 for axis in range(len(shape))])
    return gain


def centred(key, extent, width, most, cuts=(), kind=jnp.bfloat16):
    loudness = levels(key, extent, cuts, -0.22, 0.18) if cuts else 1.0
    result = jax.random.normal(key, extent, jnp.float32) * width * loudness
    return jnp.minimum(jnp.maximum(result, -most), most).astype(kind)


def setup_inputs(seed: int = 0) -> dict:
    key_of = jax.random.split(jax.random.key(seed), 7)
    activations = centred(key_of[0], (MICRO, BATCH_ROWS, D), 1.0, 6.0, ((1, 32),))
    cotangent = centred(key_of[1], (MICRO, BATCH_ROWS, D), 1.0, 6.0, ((1, 32),))
    weight = centred(key_of[2], (SECTIONS, D, D), D ** -0.5, 0.125, ((0, 8), (1, 32)))
    norm_gain = jnp.clip(1.0 + 0.18 * jax.random.normal(key_of[3], (SECTIONS, D), jnp.float32), 0.1, 1.9)
    pair_mask = draw_pair_mask(jax.random.fold_in(key_of[6], 71), 0)
    earlier_mask = draw_earlier_mask(jax.random.fold_in(key_of[6], 71), 0)
    return {"activations": activations, "cotangent": cotangent, "weight": weight, "norm_gain": norm_gain, "pair_mask": pair_mask, "earlier_mask": earlier_mask}


epsilon = 1e-06
decay_rate = 4.0
half_root = 0.7071067811865476
density_scale = 0.3989422804014327
first_table = (0, 0, 0, 1, 1, 2)
second_table = (1, 2, 3, 2, 3, 3)

def pair_ends(indices):
    leading = jnp.zeros_like(indices)
    trailing = jnp.zeros_like(indices)
    for pair_index in range(6):
        matches = indices == pair_index
        leading = jnp.where(matches, first_table[pair_index], leading)
        trailing = jnp.where(matches, second_table[pair_index], trailing)
    return (leading, trailing)

def kept_positions(indices):
    leading, trailing = pair_ends(indices)
    groups, columns = indices.shape
    positions = lax.broadcasted_iota(jnp.int32, (groups, 4, columns), 1)
    kept_mask = (positions == leading[:, None, :]) | (positions == trailing[:, None, :])
    return kept_mask.reshape(groups * 4, columns)

def section_forward(inputs, masked, gain_row):
    values = inputs.astype(jnp.float32)
    norm_scale = lax.rsqrt(lax.optimization_barrier(jnp.mean(values * values, axis=-1, keepdims=True)) + epsilon)
    normed = (values * norm_scale * gain_row).astype(jnp.bfloat16)
    preact = jnp.dot(normed, masked, preferred_element_type=jnp.float32)
    normal_cdf = 0.5 * (1.0 + lax.erf(preact * half_root))
    outputs = (values + preact * normal_cdf).astype(jnp.bfloat16)
    return (normed, preact, outputs)

def section_backward(inputs, preact, upstream, masked, gain_row):
    values = inputs.astype(jnp.float32)
    norm_scale = lax.rsqrt(lax.optimization_barrier(jnp.mean(values * values, axis=-1, keepdims=True)) + epsilon)
    normal_cdf = 0.5 * (1.0 + lax.erf(preact * half_root))
    normal_pdf = jnp.exp(-0.5 * preact * preact) * density_scale
    upstream_f = upstream.astype(jnp.float32)
    grad_pre = (upstream_f * (normal_cdf + preact * normal_pdf)).astype(jnp.bfloat16)
    grad_normed = lax.dot_general(grad_pre, masked, (((1,), (1,)), ((), ())), preferred_element_type=jnp.float32)
    scaled_grad = grad_normed * gain_row
    grad_input = norm_scale * scaled_grad - values * norm_scale ** 3 * lax.optimization_barrier(jnp.mean(scaled_grad * values, axis=-1, keepdims=True))
    return (grad_pre, (upstream_f + grad_input).astype(jnp.bfloat16))

def replica_terms(normed, grad_pre, micro_count):
    replicas = N_DP
    model_width = normed.shape[1]
    row_count = normed.shape[0] // (micro_count * replicas)
    normed_split = normed.reshape(micro_count, replicas, row_count, model_width).transpose(1, 0, 2, 3).reshape(replicas, micro_count * row_count, model_width)
    grad_split = grad_pre.reshape(micro_count, replicas, row_count, model_width).transpose(1, 0, 2, 3).reshape(replicas, micro_count * row_count, model_width)

    def add_replica(running, pieces):
        partial_term = lax.dot_general(pieces[0], pieces[1], (((0,), (0,)), ((), ())), preferred_element_type=jnp.float32)
        rounded = lax.optimization_barrier(partial_term.astype(jnp.bfloat16))
        return (running + rounded.astype(jnp.float32), None)
    running, unused = lax.scan(add_replica, jnp.zeros((model_width, model_width), jnp.float32), (normed_split, grad_split))
    return running

def reference(activations, cotangent, weight, norm_gain, pair_mask, earlier_mask):
    micro_count, batch_rows, model_width = activations.shape
    hidden = activations.reshape(micro_count * batch_rows, model_width)
    upstream = cotangent.reshape(micro_count * batch_rows, model_width)
    masked_list = []
    kept_list = []
    for section_index in range(SECTIONS):
        kept_mask = kept_positions(pair_mask[section_index])
        kept_list.append(kept_mask)
        masked_list.append(jnp.where(kept_mask, weight[section_index], jnp.zeros_like(weight[section_index])))
    saved_inputs = []
    saved_normed = []
    saved_preact = []
    for section_index in range(SECTIONS):
        saved_inputs.append(hidden)
        normed, preact, hidden = section_forward(hidden, masked_list[section_index], norm_gain[section_index])
        saved_normed.append(normed)
        saved_preact.append(preact)
    gradients = [None] * SECTIONS
    for section_index in reversed(range(SECTIONS)):
        grad_pre, upstream = section_backward(saved_inputs[section_index], saved_preact[section_index], upstream, masked_list[section_index], norm_gain[section_index])
        dense_part = replica_terms(saved_normed[section_index], grad_pre, micro_count) / math.sqrt(TOKENS)
        decay_part = jnp.where(kept_list[section_index], 0.0, weight[section_index].astype(jnp.float32))
        gradients[section_index] = dense_part + decay_rate * decay_part
    flip_list = []
    for section_index in range(SECTIONS):
        earlier_kept = kept_positions(earlier_mask[section_index])
        flip_list.append(jnp.sum(kept_list[section_index] != earlier_kept).astype(jnp.int32))
    return (jnp.stack(gradients), jnp.stack(flip_list))
```

```python
import functools
import math

import jax
import jax.numpy as jnp
from jax import lax
from jax.experimental import pallas as pl
from jax.experimental.pallas import tpu as pltpu
from jax.sharding import Mesh
from jax.sharding import PartitionSpec as P

epsilon = 1e-06
decay_rate = 4.0
half_root = 0.7071067811865476
density_scale = 0.3989422804014327

NY, NX, NC, SECTIONS = 4, 4, 2, 8
DP = ("y", "x", "core")
ROWS = 64
STREAMS = 1
BLOCK = 512
LIMIT = 24 * 1024 * 1024
bf16 = jnp.bfloat16
f32 = jnp.float32


def params(limit=LIMIT):
    return pltpu.CompilerParams(vmem_limit_bytes=limit, dimension_semantics=("arbitrary",))


def kept_planes(p):
    return (
        p < 3,
        (p == 0) | (p == 3) | (p == 4),
        (p == 1) | (p == 3) | (p == 5),
        (p == 2) | (p >= 4),
    )


def prep_kernel(rep_ref, w_ref, pair_ref, old_ref, left_ref, right_ref, flip_ref, decay_ref, work):
    del rep_ref
    groups = pair_ref.shape[0]
    lanes = work.shape[0]
    total = jnp.zeros((groups, 128), f32)
    for i in range(lanes):
        cols = slice(i * 128, (i + 1) * 128)
        work[i] = w_ref[:, cols].astype(f32)
        p = pair_ref[:, cols]
        w = [work[i, pl.ds(j, groups, stride=4), :] for j in range(4)]
        v0 = jnp.where(p < 3, w[0], jnp.where(p < 5, w[1], w[2]))
        v1 = jnp.where(p == 0, w[1], jnp.where((p == 1) | (p == 3), w[2], w[3]))
        both = jnp.concatenate([v0, v1], axis=0).astype(bf16)
        if i < lanes // 2:
            left_ref[:, cols] = both
        else:
            right_ref[:, (i - lanes // 2) * 128 : (i - lanes // 2 + 1) * 128] = both
        kept = kept_planes(p)
        old = kept_planes(old_ref[:, cols])
        for j in range(4):
            total = total + jnp.where(kept[j] != old[j], 1.0, 0.0)
            work[i, pl.ds(j, groups, stride=4), :] = jnp.where(kept[j], 0.0, w[j]) * decay_rate
        decay_ref[:, cols] = work[i]
    count = jnp.sum(jnp.sum(total, axis=0, keepdims=True), axis=1, keepdims=True)
    flip_ref[...] = jnp.broadcast_to(count, flip_ref.shape).astype(jnp.int32)


def prep(replica, weight, pairs, earlier):
    rows, width = weight.shape
    groups = rows // 4
    whole = lambda i, r: (0, 0)
    return pl.pallas_call(
        prep_kernel,
        grid_spec=pltpu.PrefetchScalarGridSpec(
            num_scalar_prefetch=1,
            grid=(1,),
            in_specs=[
                pl.BlockSpec((rows, width), whole),
                pl.BlockSpec((groups, width), lambda i, r: (r[0], 0)),
                pl.BlockSpec((groups, width), whole),
            ],
            out_specs=[
                pl.BlockSpec((2 * groups, width // 2), whole),
                pl.BlockSpec((2 * groups, width // 2), whole),
                pl.BlockSpec((8, 128), whole),
                pl.BlockSpec((rows, width), whole),
            ],
            scratch_shapes=[pltpu.VMEM((width // 128, rows, 128), f32)],
        ),
        out_shape=[
            jax.ShapeDtypeStruct((2 * groups, width // 2), bf16),
            jax.ShapeDtypeStruct((2 * groups, width // 2), bf16),
            jax.ShapeDtypeStruct((8, 128), jnp.int32),
            jax.ShapeDtypeStruct((rows, width), f32),
        ],
        compiler_params=params(),
        name="prep",
    )(replica, weight, pairs, earlier)


def expand_kernel(pos_ref, lo_ref, ro_ref, lt_ref, rt_ref, pair_ref, w_ref, work):
    core = pos_ref[2]
    lanes = work.shape[0]
    groups = work.shape[1] // 4
    for c in range(2):
        mine = core == c
        for i in range(lanes):
            cols = slice(i * 128, (i + 1) * 128)
            own, other = (lo_ref, lt_ref) if i < lanes // 2 else (ro_ref, rt_ref)
            k = i % (lanes // 2)
            both = jnp.where(
                mine,
                own[0, 0, :, k * 128 : (k + 1) * 128].astype(f32),
                other[0, 0, :, k * 128 : (k + 1) * 128].astype(f32),
            )
            v0, v1 = both[:groups], both[groups:]
            p = pair_ref[c * groups : (c + 1) * groups, cols]
            planes = (
                jnp.where(p < 3, v0, 0.0),
                jnp.where(p == 0, v1, jnp.where((p == 3) | (p == 4), v0, 0.0)),
                jnp.where(p == 5, v0, jnp.where((p == 1) | (p == 3), v1, 0.0)),
                jnp.where((p == 2) | (p >= 4), v1, 0.0),
            )
            for j in range(4):
                work[i, pl.ds(j, groups, stride=4), :] = planes[j]
            w_ref[c * 4 * groups : (c + 1) * 4 * groups, cols] = work[i].astype(bf16)


def expand(pos, left_own, right_own, left_other, right_other, pairs):
    rows, half = left_own.shape[2:]
    groups = rows // 2
    width = 2 * half

    def part(i, pos):
        return (lax.rem(pos[0] - i // NX + NY, NY), lax.rem(pos[1] - lax.rem(i, NX) + NX, NX), 0, 0)

    spec = pl.BlockSpec((1, 1, rows, half), part)
    return pl.pallas_call(
        expand_kernel,
        grid_spec=pltpu.PrefetchScalarGridSpec(
            num_scalar_prefetch=1,
            grid=(NY * NX,),
            in_specs=[spec, spec, spec, spec, pl.BlockSpec((2 * groups, width), lambda i, pos: (i, 0))],
            out_specs=pl.BlockSpec((8 * groups, width), lambda i, pos: (i, 0)),
            scratch_shapes=[pltpu.VMEM((width // 128, 4 * groups, 128), f32)],
        ),
        out_shape=jax.ShapeDtypeStruct((pairs.shape[0] * 4, width), bf16),
        compiler_params=params(),
        name="expand",
    )(pos, left_own, right_own, left_other, right_other, pairs)


def forward_kernel(
    slots, j_ref, s_ref, recv_ref, act_ref, gain_ref, w_ref, hb_in, nb_in, db_in,
    out_ref, h_ref, n_ref, d_ref,
):
    del hb_in, nb_in, db_in
    n = pl.program_id(0)
    live = (j_ref[0] >= 0) & (j_ref[0] < slots)

    @pl.when(live & (n == 0))
    def _():
        current = jnp.where(s_ref[0] == 0, act_ref[0].astype(f32), recv_ref[...].astype(f32))
        scale = lax.rsqrt(jnp.mean(current * current, axis=-1, keepdims=True) + epsilon)
        h_ref[0] = current.astype(bf16)
        n_ref[0] = (current * scale * gain_ref[...]).astype(bf16)

    @pl.when(live)
    def _():
        columns = pl.ds(pl.multiple_of(n * BLOCK, BLOCK), BLOCK)
        preact = jnp.dot(n_ref[0], w_ref[...], preferred_element_type=f32)
        cdf = 0.5 * (1.0 + lax.erf(preact * half_root))
        pdf = jnp.exp(-0.5 * preact * preact) * density_scale
        d_ref[0, :, columns] = cdf + preact * pdf
        out_ref[:, columns] = (h_ref[0, :, columns].astype(f32) + preact * cdf).astype(bf16)


def forward_step(j, s, recv, acts, gain, masked, buffers, slots, first_chunk):
    rows, width = recv.shape
    blocks = width // BLOCK
    hb, nb, db = buffers

    def slot(n, j, s):
        return (jnp.where((j[0] >= 0) & (j[0] < slots), j[0], slots), 0, 0)

    def w_block(n, j, s):
        return (0, jnp.where((j[0] >= 0) & (j[0] < slots), n, 0))

    whole = lambda n, j, s: (0, 0)
    store = pl.BlockSpec((1, rows, width), slot)
    keep = pl.BlockSpec(memory_space=pl.ANY)
    out, hb, nb, db = pl.pallas_call(
        functools.partial(forward_kernel, slots),
        grid_spec=pltpu.PrefetchScalarGridSpec(
            num_scalar_prefetch=2,
            grid=(blocks,),
            in_specs=[
                pl.BlockSpec((rows, width), whole),
                pl.BlockSpec((1, rows, width), lambda n, j, s: (first_chunk + jnp.clip(j[0], 0, slots - 1), 0, 0)),
                pl.BlockSpec((1, width), whole),
                pl.BlockSpec((width, BLOCK), w_block),
                keep, keep, keep,
            ],
            out_specs=[pl.BlockSpec((rows, width), whole), store, store, store],
        ),
        out_shape=[
            jax.ShapeDtypeStruct((rows, width), bf16),
            jax.ShapeDtypeStruct(hb.shape, hb.dtype),
            jax.ShapeDtypeStruct(nb.shape, nb.dtype),
            jax.ShapeDtypeStruct(db.shape, db.dtype),
        ],
        input_output_aliases={6: 1, 7: 2, 8: 3},
        compiler_params=params(),
        name="forward",
    )(j, s, recv, acts, gain, masked, hb, nb, db)
    return out, (hb, nb, db)


def backward_kernel(
    slots, j_ref, s_ref, recv_ref, cot_ref, gain_ref, h_ref, d_ref, w_ref, gb_in,
    out_ref, g_ref, up_ref, a_ref,
):
    del gb_in
    n = pl.program_id(0)
    live = (j_ref[0] >= 0) & (j_ref[0] < slots)

    @pl.when(live & (n == 0))
    def _():
        upstream = jnp.where(
            s_ref[0] == SECTIONS - 1, cot_ref[0].astype(f32), recv_ref[...].astype(f32)
        )
        up_ref[...] = upstream
        g_ref[0] = (upstream * d_ref[0]).astype(bf16)

    @pl.when(live)
    def _():
        columns = pl.ds(pl.multiple_of(n * BLOCK, BLOCK), BLOCK)
        grad = lax.dot_general(
            g_ref[0], w_ref[...], (((1,), (1,)), ((), ())), preferred_element_type=f32
        )
        a_ref[:, columns] = grad * gain_ref[:, columns]

    @pl.when(live & (n == pl.num_programs(0) - 1))
    def _():
        h = h_ref[0].astype(f32)
        a = a_ref[...]
        scale = lax.rsqrt(jnp.mean(h * h, axis=-1, keepdims=True) + epsilon)
        dot = jnp.mean(a * h, axis=-1, keepdims=True)
        out_ref[...] = (up_ref[...] + scale * a - h * (scale * scale * scale) * dot).astype(bf16)


def backward_step(j, s, recv, cots, gain, masked, buffers, gb, slots, first_chunk):
    rows, width = recv.shape
    blocks = width // BLOCK
    hb, _, db = buffers

    def slot(n, j, s):
        return (jnp.where((j[0] >= 0) & (j[0] < slots), j[0], slots), 0, 0)

    def w_block(n, j, s):
        return (jnp.where((j[0] >= 0) & (j[0] < slots), n, 0), 0)

    whole = lambda n, j, s: (0, 0)
    store = pl.BlockSpec((1, rows, width), slot)
    return pl.pallas_call(
        functools.partial(backward_kernel, slots),
        grid_spec=pltpu.PrefetchScalarGridSpec(
            num_scalar_prefetch=2,
            grid=(blocks,),
            in_specs=[
                pl.BlockSpec((rows, width), whole),
                pl.BlockSpec((1, rows, width), lambda n, j, s: (first_chunk + jnp.clip(j[0], 0, slots - 1), 0, 0)),
                pl.BlockSpec((1, width), whole),
                store,
                store,
                pl.BlockSpec((BLOCK, width), w_block),
                pl.BlockSpec(memory_space=pl.ANY),
            ],
            out_specs=[pl.BlockSpec((rows, width), whole), store],
            scratch_shapes=[pltpu.VMEM((rows, width), f32), pltpu.VMEM((rows, width), f32)],
        ),
        out_shape=[
            jax.ShapeDtypeStruct((rows, width), bf16),
            jax.ShapeDtypeStruct(gb.shape, gb.dtype),
        ],
        input_output_aliases={8: 1},
        compiler_params=params(),
        name="backward",
    )(j, s, recv, cots, gain, hb, db, masked, gb)


def ring(x, axis, distance):
    n = lax.axis_size(axis)
    return lax.ppermute(x, axis, [(i, (i + distance) % n) for i in range(n)])


def gather4(block, axis, direct):
    back = ring(block, axis, 1)
    ahead = ring(block, axis, -1)
    if direct:
        across = ring(block, axis, 2)
    else:
        half = block.shape[0] // 2
        across = jnp.concatenate([ring(back[:half], axis, 1), ring(ahead[half:], axis, -1)], axis=0)
    return jnp.stack([block, back, across, ahead])


def scatter4(chunks, axis, dim):
    me = lax.axis_index(axis)
    own, nxt, across, prev = [
        lax.dynamic_index_in_dim(chunks, lax.rem(me + k, 4), dim, keepdims=False) for k in range(4)
    ]
    a = ring(nxt, axis, 1)
    b = ring(prev, axis, -1)
    c = ring(across, axis, 2)
    return own.astype(f32) + a.astype(f32) + b.astype(f32) + c.astype(f32)


def token_product(x, g):
    return lax.dot_general(x, g, (((0,), (0,)), ((), ())), preferred_element_type=f32)


def body(activations, cotangent, weight, norm_gain, pair_mask, earlier_mask):
    section = lax.axis_index("section")
    y, x, core = (lax.axis_index(name) for name in DP)
    replica = (y * NX + x) * NC + core
    micro_count, row_count, width = activations.shape
    tokens = micro_count * row_count
    chunks = tokens // ROWS
    slots = chunks // STREAMS
    acts = activations.reshape(chunks, ROWS, width)
    cots = cotangent.reshape(chunks, ROWS, width)
    s = section.reshape(1).astype(jnp.int32)
    half = width // 2

    left, right, flips, decay = prep(
        replica.reshape(1).astype(jnp.int32), weight[0], pair_mask[0], earlier_mask[0]
    )

    left = gather4(left, "x", True)
    right = gather4(right, "y", True)
    rows = left.shape[1]
    left = gather4(left.reshape(4 * rows, half), "y", False).reshape(4, 4, rows, half)
    right = gather4(right.reshape(4 * rows, half), "x", False).reshape(4, 4, rows, half)
    right = jnp.swapaxes(right, 0, 1)
    pos = jnp.stack([y, x, core]).astype(jnp.int32)
    masked = expand(pos, left, right, ring(left, "core", 1), ring(right, "core", 1), pair_mask[0])

    fwd_ticks = slots + SECTIONS - 1
    zero = lambda dtype: jnp.zeros((slots + 1, ROWS, width), dtype)
    buffers = [(zero(bf16), zero(bf16), zero(f32)) for _ in range(STREAMS)]
    grads = [zero(bf16) for _ in range(STREAMS)]
    fwd = [acts[0] for _ in range(STREAMS)]
    bwd = [cots[0] for _ in range(STREAMS)]
    for tick in range(SECTIONS + fwd_ticks):
        for k in range(STREAMS):
            if tick >= SECTIONS:
                j = (tick - 2 * SECTIONS + 1 + section).reshape(1).astype(jnp.int32)
                out, grads[k] = backward_step(
                    j, s, bwd[k], cots, norm_gain, masked, buffers[k], grads[k], slots, k * slots
                )
                if tick < SECTIONS + fwd_ticks - 1:
                    bwd[k] = ring(out, "section", -1)
            if tick < fwd_ticks:
                j = (tick - section).reshape(1).astype(jnp.int32)
                out, buffers[k] = forward_step(
                    j, s, fwd[k], acts, norm_gain, masked, buffers[k], slots, k * slots
                )
                if tick < fwd_ticks - 1:
                    fwd[k] = ring(out, "section", 1)

    flat = lambda b: b[:slots].reshape(slots * ROWS, width)
    normed = jnp.concatenate([flat(b[1]) for b in buffers], axis=0)
    grad = jnp.concatenate([flat(g) for g in grads], axis=0)
    g_left, g_right = grad[:, :half], grad[:, half:]
    first = core == 0
    g_mine = jnp.where(first, g_left, g_right)
    normed_other = ring(normed, "core", 1)
    g_other = ring(jnp.where(first, g_right, g_left), "core", 1)
    quarter = half // 2
    parts = []
    for c in range(2):
        cols = slice(c * quarter, (c + 1) * quarter)
        partial = token_product(normed, g_mine[:, cols]) + token_product(normed_other, g_other[:, cols])
        parts.append(partial.astype(bf16).reshape(NY, NX, 2 * row_count, quarter))
    part_l = scatter4(parts[0], "x", 1).astype(bf16)
    part_r = scatter4(parts[1], "y", 0).astype(bf16)
    part_l = scatter4(part_l, "y", 0)
    part_r = scatter4(part_r, "x", 0)
    mine = jnp.concatenate([part_l, part_r], axis=1)
    top, bottom = mine[:row_count], mine[row_count:]
    own = jnp.where(first, top, bottom)
    other = ring(jnp.where(first, bottom, top).astype(bf16), "core", 1).astype(f32)
    total = jnp.where(
        first, jnp.concatenate([own, other], axis=1), jnp.concatenate([other, own], axis=1)
    )
    gradient = total / math.sqrt(tokens * NY * NX * NC) + decay

    count = flips + ring(flips, "core", 1)
    count = count + ring(count, "x", 1) + ring(count, "x", -1) + ring(count, "x", 2)
    count = count + ring(count, "y", 1) + ring(count, "y", -1) + ring(count, "y", 2)
    return gradient[None], count[0, :1]


def solution(mesh):
    cube = Mesh(mesh.devices.reshape(NY, NX, NC, SECTIONS), (*DP, "section"))
    placed = (
        P(None, DP, None),
        P(None, DP, None),
        P("section", DP, None),
        P("section", None),
        P("section", None, None),
        P("section", DP, None),
    )
    return jax.shard_map(
        body,
        mesh=cube,
        in_specs=placed,
        out_specs=(P("section", DP, None), P("section")),
        check_vma=False,
    )
```

```python
import functools
import math

import jax
import jax.numpy as jnp
from jax import lax
from jax.experimental import pallas as pl
from jax.experimental.pallas import tpu as pltpu
from jax.sharding import Mesh
from jax.sharding import PartitionSpec as P

epsilon = 1e-06
decay_rate = 4.0
half_root = 0.7071067811865476
density_scale = 0.3989422804014327

NY, NX, NC, SECTIONS = 4, 4, 2, 8
DP = ("y", "x", "core")
ROWS = 64
STREAMS = 1
BLOCK = 512
LIMIT = 24 * 1024 * 1024
bf16 = jnp.bfloat16
f32 = jnp.float32


def params(limit=LIMIT):
    return pltpu.CompilerParams(vmem_limit_bytes=limit, dimension_semantics=("arbitrary",))


def kept_planes(p):
    return (
        p < 3,
        (p == 0) | (p == 3) | (p == 4),
        (p == 1) | (p == 3) | (p == 5),
        (p == 2) | (p >= 4),
    )


def prep_kernel(rep_ref, w_ref, pair_ref, old_ref, left_ref, right_ref, flip_ref, decay_ref, work):
    del rep_ref
    groups = pair_ref.shape[0]
    lanes = work.shape[0]
    total = jnp.zeros((groups, 128), f32)
    for i in range(lanes):
        cols = slice(i * 128, (i + 1) * 128)
        work[i] = w_ref[:, cols].astype(f32)
        p = pair_ref[:, cols]
        w = [work[i, pl.ds(j, groups, stride=4), :] for j in range(4)]
        v0 = jnp.where(p < 3, w[0], jnp.where(p < 5, w[1], w[2]))
        v1 = jnp.where(p == 0, w[1], jnp.where((p == 1) | (p == 3), w[2], w[3]))
        both = jnp.concatenate([v0, v1], axis=0).astype(bf16)
        if i < lanes // 2:
            left_ref[:, cols] = both
        else:
            right_ref[:, (i - lanes // 2) * 128 : (i - lanes // 2 + 1) * 128] = both
        kept = kept_planes(p)
        old = kept_planes(old_ref[:, cols])
        for j in range(4):
            total = total + jnp.where(kept[j] != old[j], 1.0, 0.0)
            work[i, pl.ds(j, groups, stride=4), :] = jnp.where(kept[j], 0.0, w[j]) * decay_rate
        decay_ref[:, cols] = work[i]
    count = jnp.sum(jnp.sum(total, axis=0, keepdims=True), axis=1, keepdims=True)
    flip_ref[...] = jnp.broadcast_to(count, flip_ref.shape).astype(jnp.int32)


def prep(replica, weight, pairs, earlier):
    rows, width = weight.shape
    groups = rows // 4
    whole = lambda i, r: (0, 0)
    return pl.pallas_call(
        prep_kernel,
        grid_spec=pltpu.PrefetchScalarGridSpec(
            num_scalar_prefetch=1,
            grid=(1,),
            in_specs=[
                pl.BlockSpec((rows, width), whole),
                pl.BlockSpec((groups, width), lambda i, r: (r[0], 0)),
                pl.BlockSpec((groups, width), whole),
            ],
            out_specs=[
                pl.BlockSpec((2 * groups, width // 2), whole),
                pl.BlockSpec((2 * groups, width // 2), whole),
                pl.BlockSpec((8, 128), whole),
                pl.BlockSpec((rows, width), whole),
            ],
            scratch_shapes=[pltpu.VMEM((width // 128, rows, 128), f32)],
        ),
        out_shape=[
            jax.ShapeDtypeStruct((2 * groups, width // 2), bf16),
            jax.ShapeDtypeStruct((2 * groups, width // 2), bf16),
            jax.ShapeDtypeStruct((8, 128), jnp.int32),
            jax.ShapeDtypeStruct((rows, width), f32),
        ],
        compiler_params=params(),
        name="prep",
    )(replica, weight, pairs, earlier)


def expand_kernel(pos_ref, lo_ref, ro_ref, lt_ref, rt_ref, pair_ref, w_ref, work):
    core = pos_ref[2]
    lanes = work.shape[0]
    groups = work.shape[1] // 4
    for c in range(2):
        mine = core == c
        for i in range(lanes):
            cols = slice(i * 128, (i + 1) * 128)
            own, other = (lo_ref, lt_ref) if i < lanes // 2 else (ro_ref, rt_ref)
            k = i % (lanes // 2)
            both = jnp.where(
                mine,
                own[0, 0, :, k * 128 : (k + 1) * 128].astype(f32),
                other[0, 0, :, k * 128 : (k + 1) * 128].astype(f32),
            )
            v0, v1 = both[:groups], both[groups:]
            p = pair_ref[c * groups : (c + 1) * groups, cols]
            planes = (
                jnp.where(p < 3, v0, 0.0),
                jnp.where(p == 0, v1, jnp.where((p == 3) | (p == 4), v0, 0.0)),
                jnp.where(p == 5, v0, jnp.where((p == 1) | (p == 3), v1, 0.0)),
                jnp.where((p == 2) | (p >= 4), v1, 0.0),
            )
            for j in range(4):
                work[i, pl.ds(j, groups, stride=4), :] = planes[j]
            w_ref[c * 4 * groups : (c + 1) * 4 * groups, cols] = work[i].astype(bf16)


def expand(pos, left_own, right_own, left_other, right_other, pairs):
    rows, half = left_own.shape[2:]
    groups = rows // 2
    width = 2 * half

    def part(i, pos):
        return (lax.rem(pos[0] - i // NX + NY, NY), lax.rem(pos[1] - lax.rem(i, NX) + NX, NX), 0, 0)

    spec = pl.BlockSpec((1, 1, rows, half), part)
    return pl.pallas_call(
        expand_kernel,
        grid_spec=pltpu.PrefetchScalarGridSpec(
            num_scalar_prefetch=1,
            grid=(NY * NX,),
            in_specs=[spec, spec, spec, spec, pl.BlockSpec((2 * groups, width), lambda i, pos: (i, 0))],
            out_specs=pl.BlockSpec((8 * groups, width), lambda i, pos: (i, 0)),
            scratch_shapes=[pltpu.VMEM((width // 128, 4 * groups, 128), f32)],
        ),
        out_shape=jax.ShapeDtypeStruct((pairs.shape[0] * 4, width), bf16),
        compiler_params=params(),
        name="expand",
    )(pos, left_own, right_own, left_other, right_other, pairs)


def forward_slot(t, s):
    return t[0] - s[0]


def backward_slot(t, s):
    return t[0] - 2 * SECTIONS + 1 + s[0]


def is_live(j, slots):
    return (j >= 0) & (j < slots)


def forward_kernel(
    slots, t_ref, s_ref, recv_ref, act_ref, gain_ref, w_ref, hb_in, nb_in, db_in,
    out_ref, h_ref, n_ref, d_ref,
):
    del hb_in, nb_in, db_in
    n = pl.program_id(0)
    live = is_live(forward_slot(t_ref, s_ref), slots)

    @pl.when(live & (n == 0))
    def _():
        current = jnp.where(s_ref[0] == 0, act_ref[0].astype(f32), recv_ref[...].astype(f32))
        scale = lax.rsqrt(jnp.mean(current * current, axis=-1, keepdims=True) + epsilon)
        h_ref[0] = current.astype(bf16)
        n_ref[0] = (current * scale * gain_ref[...]).astype(bf16)

    @pl.when(live)
    def _():
        columns = pl.ds(pl.multiple_of(n * BLOCK, BLOCK), BLOCK)
        preact = jnp.dot(n_ref[0], w_ref[...], preferred_element_type=f32)
        cdf = 0.5 * (1.0 + lax.erf(preact * half_root))
        pdf = jnp.exp(-0.5 * preact * preact) * density_scale
        d_ref[0, :, columns] = cdf + preact * pdf
        out_ref[:, columns] = (h_ref[0, :, columns].astype(f32) + preact * cdf).astype(bf16)


def forward_step(t, s, recv, acts, gain, masked, buffers, slots, first_chunk):
    rows, width = recv.shape
    blocks = width // BLOCK
    hb, nb, db = buffers

    def slot(n, t, s):
        j = forward_slot(t, s)
        return (jnp.where(is_live(j, slots), j, slots), 0, 0)

    def w_block(n, t, s):
        return (0, jnp.where(is_live(forward_slot(t, s), slots), n, 0))

    def chunk(n, t, s):
        return (first_chunk + jnp.clip(forward_slot(t, s), 0, slots - 1), 0, 0)

    whole = lambda n, t, s: (0, 0)
    store = pl.BlockSpec((1, rows, width), slot)
    keep = pl.BlockSpec(memory_space=pl.ANY)
    out, hb, nb, db = pl.pallas_call(
        functools.partial(forward_kernel, slots),
        grid_spec=pltpu.PrefetchScalarGridSpec(
            num_scalar_prefetch=2,
            grid=(blocks,),
            in_specs=[
                pl.BlockSpec((rows, width), whole),
                pl.BlockSpec((1, rows, width), chunk),
                pl.BlockSpec((1, width), whole),
                pl.BlockSpec((width, BLOCK), w_block),
                keep, keep, keep,
            ],
            out_specs=[pl.BlockSpec((rows, width), whole), store, store, store],
        ),
        out_shape=[
            jax.ShapeDtypeStruct((rows, width), bf16),
            jax.ShapeDtypeStruct(hb.shape, hb.dtype),
            jax.ShapeDtypeStruct(nb.shape, nb.dtype),
            jax.ShapeDtypeStruct(db.shape, db.dtype),
        ],
        input_output_aliases={6: 1, 7: 2, 8: 3},
        compiler_params=params(),
        name="forward",
    )(t, s, recv, acts, gain, masked, hb, nb, db)
    return out, (hb, nb, db)


def backward_kernel(
    slots, t_ref, s_ref, recv_ref, cot_ref, gain_ref, h_ref, d_ref, w_ref, gb_in,
    out_ref, g_ref, up_ref, a_ref,
):
    del gb_in
    n = pl.program_id(0)
    live = is_live(backward_slot(t_ref, s_ref), slots)

    @pl.when(live & (n == 0))
    def _():
        upstream = jnp.where(
            s_ref[0] == SECTIONS - 1, cot_ref[0].astype(f32), recv_ref[...].astype(f32)
        )
        up_ref[...] = upstream
        g_ref[0] = (upstream * d_ref[0]).astype(bf16)

    @pl.when(live)
    def _():
        columns = pl.ds(pl.multiple_of(n * BLOCK, BLOCK), BLOCK)
        grad = lax.dot_general(
            g_ref[0], w_ref[...], (((1,), (1,)), ((), ())), preferred_element_type=f32
        )
        a_ref[:, columns] = grad * gain_ref[:, columns]

    @pl.when(live & (n == pl.num_programs(0) - 1))
    def _():
        h = h_ref[0].astype(f32)
        a = a_ref[...]
        scale = lax.rsqrt(jnp.mean(h * h, axis=-1, keepdims=True) + epsilon)
        dot = jnp.mean(a * h, axis=-1, keepdims=True)
        out_ref[...] = (up_ref[...] + scale * a - h * (scale * scale * scale) * dot).astype(bf16)


def backward_step(t, s, recv, cots, gain, masked, buffers, gb, slots, first_chunk):
    rows, width = recv.shape
    blocks = width // BLOCK
    hb, _, db = buffers

    def slot(n, t, s):
        j = backward_slot(t, s)
        return (jnp.where(is_live(j, slots), j, slots), 0, 0)

    def w_block(n, t, s):
        return (jnp.where(is_live(backward_slot(t, s), slots), n, 0), 0)

    def chunk(n, t, s):
        return (first_chunk + jnp.clip(backward_slot(t, s), 0, slots - 1), 0, 0)

    whole = lambda n, t, s: (0, 0)
    store = pl.BlockSpec((1, rows, width), slot)
    return pl.pallas_call(
        functools.partial(backward_kernel, slots),
        grid_spec=pltpu.PrefetchScalarGridSpec(
            num_scalar_prefetch=2,
            grid=(blocks,),
            in_specs=[
                pl.BlockSpec((rows, width), whole),
                pl.BlockSpec((1, rows, width), chunk),
                pl.BlockSpec((1, width), whole),
                store,
                store,
                pl.BlockSpec((BLOCK, width), w_block),
                pl.BlockSpec(memory_space=pl.ANY),
            ],
            out_specs=[pl.BlockSpec((rows, width), whole), store],
            scratch_shapes=[pltpu.VMEM((rows, width), f32), pltpu.VMEM((rows, width), f32)],
        ),
        out_shape=[
            jax.ShapeDtypeStruct((rows, width), bf16),
            jax.ShapeDtypeStruct(gb.shape, gb.dtype),
        ],
        input_output_aliases={8: 1},
        compiler_params=params(),
        name="backward",
    )(t, s, recv, cots, gain, hb, db, masked, gb)


def ring(x, axis, distance):
    n = lax.axis_size(axis)
    return lax.ppermute(x, axis, [(i, (i + distance) % n) for i in range(n)])


def gather4(block, axis, direct):
    back = ring(block, axis, 1)
    ahead = ring(block, axis, -1)
    if direct:
        across = ring(block, axis, 2)
    else:
        half = block.shape[0] // 2
        across = jnp.concatenate([ring(back[:half], axis, 1), ring(ahead[half:], axis, -1)], axis=0)
    return jnp.stack([block, back, across, ahead])


def scatter4(chunks, me, axis, dim):
    own, nxt, across, prev = [
        lax.dynamic_index_in_dim(chunks, lax.rem(me + k, 4), dim, keepdims=False) for k in range(4)
    ]
    a = ring(nxt, axis, 1)
    b = ring(prev, axis, -1)
    c = ring(across, axis, 2)
    return own.astype(f32) + a.astype(f32) + b.astype(f32) + c.astype(f32)


def token_product(x, g):
    return lax.dot_general(x, g, (((0,), (0,)), ((), ())), preferred_element_type=f32)


def body(activations, cotangent, weight, norm_gain, pair_mask, earlier_mask):
    section = lax.axis_index("section")
    y, x, core = (lax.axis_index(name) for name in DP)
    replica = (y * NX + x) * NC + core
    micro_count, row_count, width = activations.shape
    tokens = micro_count * row_count
    chunks = tokens // ROWS
    slots = chunks // STREAMS
    acts = activations.reshape(chunks, ROWS, width)
    cots = cotangent.reshape(chunks, ROWS, width)
    s = section.reshape(1).astype(jnp.int32)
    half = width // 2

    left, right, flips, decay = prep(
        replica.reshape(1).astype(jnp.int32), weight[0], pair_mask[0], earlier_mask[0]
    )

    left = gather4(left, "x", True)
    right = gather4(right, "y", True)
    rows = left.shape[1]
    left = gather4(left.reshape(4 * rows, half), "y", False).reshape(4, 4, rows, half)
    right = gather4(right.reshape(4 * rows, half), "x", False).reshape(4, 4, rows, half)
    right = jnp.swapaxes(right, 0, 1)
    pos = jnp.stack([y, x, core]).astype(jnp.int32)
    masked = expand(pos, left, right, ring(left, "core", 1), ring(right, "core", 1), pair_mask[0])

    fwd_ticks = slots + SECTIONS - 1
    zero = lambda dtype: jnp.zeros((slots + 1, ROWS, width), dtype)
    buffers = [(zero(bf16), zero(bf16), zero(f32)) for _ in range(STREAMS)]
    grads = [zero(bf16) for _ in range(STREAMS)]
    fwd = [acts[0] for _ in range(STREAMS)]
    bwd = [cots[0] for _ in range(STREAMS)]
    for tick in range(SECTIONS + fwd_ticks):
        now = jnp.full((1,), tick, jnp.int32)
        for k in range(STREAMS):
            if tick >= SECTIONS:
                out, grads[k] = backward_step(
                    now, s, bwd[k], cots, norm_gain, masked, buffers[k], grads[k], slots, k * slots
                )
                if tick < SECTIONS + fwd_ticks - 1:
                    bwd[k] = ring(out, "section", -1)
            if tick < fwd_ticks:
                out, buffers[k] = forward_step(
                    now, s, fwd[k], acts, norm_gain, masked, buffers[k], slots, k * slots
                )
                if tick < fwd_ticks - 1:
                    fwd[k] = ring(out, "section", 1)

    grads, core, y, x = lax.optimization_barrier((grads, core, y, x))
    flat = lambda b: b[:slots].reshape(slots * ROWS, width)
    normed = jnp.concatenate([flat(b[1]) for b in buffers], axis=0)
    grad = jnp.concatenate([flat(g) for g in grads], axis=0)
    g_left, g_right = grad[:, :half], grad[:, half:]
    first = core == 0
    g_mine = jnp.where(first, g_left, g_right)
    normed_other = ring(normed, "core", 1)
    g_other = ring(jnp.where(first, g_right, g_left), "core", 1)
    quarter = half // 2
    parts = []
    for c in range(2):
        cols = slice(c * quarter, (c + 1) * quarter)
        partial = token_product(normed, g_mine[:, cols]) + token_product(normed_other, g_other[:, cols])
        parts.append(partial.astype(bf16).reshape(NY, NX, 2 * row_count, quarter))
    part_l = scatter4(parts[0], x, "x", 1).astype(bf16)
    part_r = scatter4(parts[1], y, "y", 0).astype(bf16)
    part_l = scatter4(part_l, y, "y", 0)
    part_r = scatter4(part_r, x, "x", 0)
    mine = jnp.concatenate([part_l, part_r], axis=1)
    top, bottom = mine[:row_count], mine[row_count:]
    own = jnp.where(first, top, bottom)
    other = ring(jnp.where(first, bottom, top).astype(bf16), "core", 1).astype(f32)
    total = jnp.where(
        first, jnp.concatenate([own, other], axis=1), jnp.concatenate([other, own], axis=1)
    )
    gradient = total / math.sqrt(tokens * NY * NX * NC) + decay

    count = flips + ring(flips, "core", 1)
    count = count + ring(count, "x", 1) + ring(count, "x", -1) + ring(count, "x", 2)
    count = count + ring(count, "y", 1) + ring(count, "y", -1) + ring(count, "y", 2)
    return gradient[None], count[0, :1]


def solution(mesh):
    cube = Mesh(mesh.devices.reshape(NY, NX, NC, SECTIONS), (*DP, "section"))
    placed = (
        P(None, DP, None),
        P(None, DP, None),
        P("section", DP, None),
        P("section", None),
        P("section", None, None),
        P("section", DP, None),
    )
    return jax.shard_map(
        body,
        mesh=cube,
        in_specs=placed,
        out_specs=(P("section", DP, None), P("section")),
        check_vma=False,
    )
```

```python
import functools
import math

import jax
import jax.numpy as jnp
from jax import lax
from jax.experimental import pallas as pl
from jax.experimental.pallas import tpu as pltpu
from jax.sharding import Mesh
from jax.sharding import PartitionSpec as P

epsilon = 1e-06
decay_rate = 4.0
half_root = 0.7071067811865476
density_scale = 0.3989422804014327

NY, NX, NC, SECTIONS = 4, 4, 2, 8
DP = ("y", "x", "core")
ROWS = 32
STREAMS = 2
BLOCK = 512
LIMIT = 12 * 1024 * 1024
bf16 = jnp.bfloat16
f32 = jnp.float32


def params(limit=LIMIT):
    return pltpu.CompilerParams(vmem_limit_bytes=limit, dimension_semantics=("arbitrary",))


def kept_planes(p):
    return (
        p < 3,
        (p == 0) | (p == 3) | (p == 4),
        (p == 1) | (p == 3) | (p == 5),
        (p == 2) | (p >= 4),
    )


def prep_kernel(rep_ref, w_ref, pair_ref, old_ref, left_ref, right_ref, flip_ref, decay_ref, work):
    del rep_ref
    groups = pair_ref.shape[0]
    lanes = work.shape[0]
    total = jnp.zeros((groups, 128), f32)
    for i in range(lanes):
        cols = slice(i * 128, (i + 1) * 128)
        work[i] = w_ref[:, cols].astype(f32)
        p = pair_ref[:, cols]
        w = [work[i, pl.ds(j, groups, stride=4), :] for j in range(4)]
        v0 = jnp.where(p < 3, w[0], jnp.where(p < 5, w[1], w[2]))
        v1 = jnp.where(p == 0, w[1], jnp.where((p == 1) | (p == 3), w[2], w[3]))
        both = jnp.concatenate([v0, v1], axis=0).astype(bf16)
        if i < lanes // 2:
            left_ref[:, cols] = both
        else:
            right_ref[:, (i - lanes // 2) * 128 : (i - lanes // 2 + 1) * 128] = both
        kept = kept_planes(p)
        old = kept_planes(old_ref[:, cols])
        for j in range(4):
            total = total + jnp.where(kept[j] != old[j], 1.0, 0.0)
            work[i, pl.ds(j, groups, stride=4), :] = jnp.where(kept[j], 0.0, w[j]) * decay_rate
        decay_ref[:, cols] = work[i]
    count = jnp.sum(jnp.sum(total, axis=0, keepdims=True), axis=1, keepdims=True)
    flip_ref[...] = jnp.broadcast_to(count, flip_ref.shape).astype(jnp.int32)


def prep(replica, weight, pairs, earlier):
    rows, width = weight.shape
    groups = rows // 4
    whole = lambda i, r: (0, 0)
    return pl.pallas_call(
        prep_kernel,
        grid_spec=pltpu.PrefetchScalarGridSpec(
            num_scalar_prefetch=1,
            grid=(1,),
            in_specs=[
                pl.BlockSpec((rows, width), whole),
                pl.BlockSpec((groups, width), lambda i, r: (r[0], 0)),
                pl.BlockSpec((groups, width), whole),
            ],
            out_specs=[
                pl.BlockSpec((2 * groups, width // 2), whole),
                pl.BlockSpec((2 * groups, width // 2), whole),
                pl.BlockSpec((8, 128), whole),
                pl.BlockSpec((rows, width), whole),
            ],
            scratch_shapes=[pltpu.VMEM((width // 128, rows, 128), f32)],
        ),
        out_shape=[
            jax.ShapeDtypeStruct((2 * groups, width // 2), bf16),
            jax.ShapeDtypeStruct((2 * groups, width // 2), bf16),
            jax.ShapeDtypeStruct((8, 128), jnp.int32),
            jax.ShapeDtypeStruct((rows, width), f32),
        ],
        compiler_params=params(),
        name="prep",
    )(replica, weight, pairs, earlier)


def expand_kernel(pos_ref, lo_ref, ro_ref, lt_ref, rt_ref, pair_ref, w_ref, work):
    core = pos_ref[2]
    lanes = work.shape[0]
    groups = work.shape[1] // 4
    for c in range(2):
        mine = core == c
        for i in range(lanes):
            cols = slice(i * 128, (i + 1) * 128)
            own, other = (lo_ref, lt_ref) if i < lanes // 2 else (ro_ref, rt_ref)
            k = i % (lanes // 2)
            both = jnp.where(
                mine,
                own[0, 0, :, k * 128 : (k + 1) * 128].astype(f32),
                other[0, 0, :, k * 128 : (k + 1) * 128].astype(f32),
            )
            v0, v1 = both[:groups], both[groups:]
            p = pair_ref[c * groups : (c + 1) * groups, cols]
            planes = (
                jnp.where(p < 3, v0, 0.0),
                jnp.where(p == 0, v1, jnp.where((p == 3) | (p == 4), v0, 0.0)),
                jnp.where(p == 5, v0, jnp.where((p == 1) | (p == 3), v1, 0.0)),
                jnp.where((p == 2) | (p >= 4), v1, 0.0),
            )
            for j in range(4):
                work[i, pl.ds(j, groups, stride=4), :] = planes[j]
            w_ref[c * 4 * groups : (c + 1) * 4 * groups, cols] = work[i].astype(bf16)


def expand(pos, left_own, right_own, left_other, right_other, pairs):
    rows, half = left_own.shape[2:]
    groups = rows // 2
    width = 2 * half

    def part(i, pos):
        return (lax.rem(pos[0] - i // NX + NY, NY), lax.rem(pos[1] - lax.rem(i, NX) + NX, NX), 0, 0)

    spec = pl.BlockSpec((1, 1, rows, half), part)
    return pl.pallas_call(
        expand_kernel,
        grid_spec=pltpu.PrefetchScalarGridSpec(
            num_scalar_prefetch=1,
            grid=(NY * NX,),
            in_specs=[spec, spec, spec, spec, pl.BlockSpec((2 * groups, width), lambda i, pos: (i, 0))],
            out_specs=pl.BlockSpec((8 * groups, width), lambda i, pos: (i, 0)),
            scratch_shapes=[pltpu.VMEM((width // 128, 4 * groups, 128), f32)],
        ),
        out_shape=jax.ShapeDtypeStruct((pairs.shape[0] * 4, width), bf16),
        compiler_params=params(),
        name="expand",
    )(pos, left_own, right_own, left_other, right_other, pairs)


def forward_slot(t, s):
    return t[0] - s[0]


def backward_slot(t, s):
    return t[0] - 2 * SECTIONS + 1 + s[0]


def is_live(j, slots):
    return (j >= 0) & (j < slots)


def forward_kernel(
    slots, t_ref, s_ref, recv_ref, act_ref, gain_ref, w_ref, hb_in, nb_in, db_in,
    out_ref, h_ref, n_ref, d_ref,
):
    del hb_in, nb_in, db_in
    n = pl.program_id(0)
    live = is_live(forward_slot(t_ref, s_ref), slots)

    @pl.when(live & (n == 0))
    def _():
        current = jnp.where(s_ref[0] == 0, act_ref[0].astype(f32), recv_ref[...].astype(f32))
        scale = lax.rsqrt(jnp.mean(current * current, axis=-1, keepdims=True) + epsilon)
        h_ref[0] = current.astype(bf16)
        n_ref[0] = (current * scale * gain_ref[...]).astype(bf16)

    @pl.when(live)
    def _():
        columns = pl.ds(pl.multiple_of(n * BLOCK, BLOCK), BLOCK)
        preact = jnp.dot(n_ref[0], w_ref[...], preferred_element_type=f32)
        cdf = 0.5 * (1.0 + lax.erf(preact * half_root))
        pdf = jnp.exp(-0.5 * preact * preact) * density_scale
        d_ref[0, :, columns] = cdf + preact * pdf
        out_ref[:, columns] = (h_ref[0, :, columns].astype(f32) + preact * cdf).astype(bf16)


def forward_step(t, s, recv, acts, gain, masked, buffers, slots, first_chunk):
    rows, width = recv.shape
    blocks = width // BLOCK
    hb, nb, db = buffers

    def slot(n, t, s):
        j = forward_slot(t, s)
        return (jnp.where(is_live(j, slots), first_chunk + j, STREAMS * slots), 0, 0)

    def w_block(n, t, s):
        return (0, jnp.where(is_live(forward_slot(t, s), slots), n, 0))

    def chunk(n, t, s):
        return (first_chunk + jnp.clip(forward_slot(t, s), 0, slots - 1), 0, 0)

    whole = lambda n, t, s: (0, 0)
    store = pl.BlockSpec((1, rows, width), slot)
    keep = pl.BlockSpec(memory_space=pl.ANY)
    out, hb, nb, db = pl.pallas_call(
        functools.partial(forward_kernel, slots),
        grid_spec=pltpu.PrefetchScalarGridSpec(
            num_scalar_prefetch=2,
            grid=(blocks,),
            in_specs=[
                pl.BlockSpec((rows, width), whole),
                pl.BlockSpec((1, rows, width), chunk),
                pl.BlockSpec((1, width), whole),
                pl.BlockSpec((width, BLOCK), w_block),
                keep, keep, keep,
            ],
            out_specs=[pl.BlockSpec((rows, width), whole), store, store, store],
        ),
        out_shape=[
            jax.ShapeDtypeStruct((rows, width), bf16),
            jax.ShapeDtypeStruct(hb.shape, hb.dtype),
            jax.ShapeDtypeStruct(nb.shape, nb.dtype),
            jax.ShapeDtypeStruct(db.shape, db.dtype),
        ],
        input_output_aliases={6: 1, 7: 2, 8: 3},
        compiler_params=params(),
        name="forward",
    )(t, s, recv, acts, gain, masked, hb, nb, db)
    return out, (hb, nb, db)


def backward_kernel(
    slots, t_ref, s_ref, recv_ref, cot_ref, gain_ref, h_ref, d_ref, w_ref, gb_in,
    out_ref, g_ref, up_ref, a_ref,
):
    del gb_in
    n = pl.program_id(0)
    live = is_live(backward_slot(t_ref, s_ref), slots)

    @pl.when(live & (n == 0))
    def _():
        upstream = jnp.where(
            s_ref[0] == SECTIONS - 1, cot_ref[0].astype(f32), recv_ref[...].astype(f32)
        )
        up_ref[...] = upstream
        g_ref[0] = (upstream * d_ref[0]).astype(bf16)

    @pl.when(live)
    def _():
        columns = pl.ds(pl.multiple_of(n * BLOCK, BLOCK), BLOCK)
        grad = lax.dot_general(
            g_ref[0], w_ref[...], (((1,), (1,)), ((), ())), preferred_element_type=f32
        )
        a_ref[:, columns] = grad * gain_ref[:, columns]

    @pl.when(live & (n == pl.num_programs(0) - 1))
    def _():
        h = h_ref[0].astype(f32)
        a = a_ref[...]
        scale = lax.rsqrt(jnp.mean(h * h, axis=-1, keepdims=True) + epsilon)
        dot = jnp.mean(a * h, axis=-1, keepdims=True)
        out_ref[...] = (up_ref[...] + scale * a - h * (scale * scale * scale) * dot).astype(bf16)


def backward_step(t, s, recv, cots, gain, masked, buffers, gb, slots, first_chunk):
    rows, width = recv.shape
    blocks = width // BLOCK
    hb, _, db = buffers

    def slot(n, t, s):
        j = backward_slot(t, s)
        return (jnp.where(is_live(j, slots), first_chunk + j, STREAMS * slots), 0, 0)

    def w_block(n, t, s):
        return (jnp.where(is_live(backward_slot(t, s), slots), n, 0), 0)

    def chunk(n, t, s):
        return (first_chunk + jnp.clip(backward_slot(t, s), 0, slots - 1), 0, 0)

    whole = lambda n, t, s: (0, 0)
    store = pl.BlockSpec((1, rows, width), slot)
    return pl.pallas_call(
        functools.partial(backward_kernel, slots),
        grid_spec=pltpu.PrefetchScalarGridSpec(
            num_scalar_prefetch=2,
            grid=(blocks,),
            in_specs=[
                pl.BlockSpec((rows, width), whole),
                pl.BlockSpec((1, rows, width), chunk),
                pl.BlockSpec((1, width), whole),
                store,
                store,
                pl.BlockSpec((BLOCK, width), w_block),
                pl.BlockSpec(memory_space=pl.ANY),
            ],
            out_specs=[pl.BlockSpec((rows, width), whole), store],
            scratch_shapes=[pltpu.VMEM((rows, width), f32), pltpu.VMEM((rows, width), f32)],
        ),
        out_shape=[
            jax.ShapeDtypeStruct((rows, width), bf16),
            jax.ShapeDtypeStruct(gb.shape, gb.dtype),
        ],
        input_output_aliases={8: 1},
        compiler_params=params(),
        name="backward",
    )(t, s, recv, cots, gain, hb, db, masked, gb)


def ring(x, axis, distance):
    n = lax.axis_size(axis)
    return lax.ppermute(x, axis, [(i, (i + distance) % n) for i in range(n)])


def gather4(block, axis, direct):
    back = ring(block, axis, 1)
    ahead = ring(block, axis, -1)
    if direct:
        across = ring(block, axis, 2)
    else:
        half = block.shape[0] // 2
        across = jnp.concatenate([ring(back[:half], axis, 1), ring(ahead[half:], axis, -1)], axis=0)
    return jnp.stack([block, back, across, ahead])


def scatter4(chunks, me, axis, dim):
    own, nxt, across, prev = [
        lax.dynamic_index_in_dim(chunks, lax.rem(me + k, 4), dim, keepdims=False) for k in range(4)
    ]
    a = ring(nxt, axis, 1)
    b = ring(prev, axis, -1)
    c = ring(across, axis, 2)
    return own.astype(f32) + a.astype(f32) + b.astype(f32) + c.astype(f32)


def token_product(x, g):
    return lax.dot_general(x, g, (((0,), (0,)), ((), ())), preferred_element_type=f32)


def body(activations, cotangent, weight, norm_gain, pair_mask, earlier_mask):
    section = lax.axis_index("section")
    y, x, core = (lax.axis_index(name) for name in DP)
    replica = (y * NX + x) * NC + core
    micro_count, row_count, width = activations.shape
    tokens = micro_count * row_count
    chunks = tokens // ROWS
    slots = chunks // STREAMS
    acts = activations.reshape(chunks, ROWS, width)
    cots = cotangent.reshape(chunks, ROWS, width)
    s = section.reshape(1).astype(jnp.int32)
    half = width // 2

    left, right, flips, decay = prep(
        replica.reshape(1).astype(jnp.int32), weight[0], pair_mask[0], earlier_mask[0]
    )

    left = gather4(left, "x", True)
    right = gather4(right, "y", True)
    rows = left.shape[1]
    left = gather4(left.reshape(4 * rows, half), "y", False).reshape(4, 4, rows, half)
    right = gather4(right.reshape(4 * rows, half), "x", False).reshape(4, 4, rows, half)
    right = jnp.swapaxes(right, 0, 1)
    pos = jnp.stack([y, x, core]).astype(jnp.int32)
    masked = expand(pos, left, right, ring(left, "core", 1), ring(right, "core", 1), pair_mask[0])

    fwd_ticks = slots + SECTIONS - 1
    zero = lambda dtype: jnp.zeros((chunks + 1, ROWS, width), dtype)
    buffers = (zero(bf16), zero(bf16), zero(f32))
    grads = zero(bf16)
    fwd = [acts[0] for _ in range(STREAMS)]
    bwd = [cots[0] for _ in range(STREAMS)]
    for tick in range(SECTIONS + fwd_ticks):
        now = jnp.full((1,), tick, jnp.int32)
        for k in range(STREAMS):
            if tick >= SECTIONS:
                out, grads = backward_step(
                    now, s, bwd[k], cots, norm_gain, masked, buffers, grads, slots, k * slots
                )
                if tick < SECTIONS + fwd_ticks - 1:
                    bwd[k] = ring(out, "section", -1)
            if tick < fwd_ticks:
                out, buffers = forward_step(
                    now, s, fwd[k], acts, norm_gain, masked, buffers, slots, k * slots
                )
                if tick < fwd_ticks - 1:
                    fwd[k] = ring(out, "section", 1)

    grads, core, y, x = lax.optimization_barrier((grads, core, y, x))
    normed = buffers[1][:chunks].reshape(tokens, width)
    grad = grads[:chunks].reshape(tokens, width)
    g_left, g_right = grad[:, :half], grad[:, half:]
    first = core == 0
    g_mine = jnp.where(first, g_left, g_right)
    normed_other = ring(normed, "core", 1)
    g_other = ring(jnp.where(first, g_right, g_left), "core", 1)
    quarter = half // 2
    parts = []
    for c in range(2):
        cols = slice(c * quarter, (c + 1) * quarter)
        partial = token_product(normed, g_mine[:, cols]) + token_product(normed_other, g_other[:, cols])
        parts.append(partial.astype(bf16).reshape(NY, NX, 2 * row_count, quarter))
    part_l = scatter4(parts[0], x, "x", 1).astype(bf16)
    part_r = scatter4(parts[1], y, "y", 0).astype(bf16)
    part_l = scatter4(part_l, y, "y", 0)
    part_r = scatter4(part_r, x, "x", 0)
    mine = jnp.concatenate([part_l, part_r], axis=1)
    top, bottom = mine[:row_count], mine[row_count:]
    own = jnp.where(first, top, bottom)
    other = ring(jnp.where(first, bottom, top).astype(bf16), "core", 1).astype(f32)
    total = jnp.where(
        first, jnp.concatenate([own, other], axis=1), jnp.concatenate([other, own], axis=1)
    )
    gradient = total / math.sqrt(tokens * NY * NX * NC) + decay

    count = flips + ring(flips, "core", 1)
    count = count + ring(count, "x", 1) + ring(count, "x", -1) + ring(count, "x", 2)
    count = count + ring(count, "y", 1) + ring(count, "y", -1) + ring(count, "y", 2)
    return gradient[None], count[0, :1]


def solution(mesh):
    cube = Mesh(mesh.devices.reshape(NY, NX, NC, SECTIONS), (*DP, "section"))
    placed = (
        P(None, DP, None),
        P(None, DP, None),
        P("section", DP, None),
        P("section", None),
        P("section", None, None),
        P("section", DP, None),
    )
    return jax.shard_map(
        body,
        mesh=cube,
        in_specs=placed,
        out_specs=(P("section", DP, None), P("section")),
        check_vma=False,
    )
```

```python
import functools
import math

import jax
import jax.numpy as jnp
from jax import lax
from jax.experimental import pallas as pl
from jax.experimental.pallas import tpu as pltpu
from jax.sharding import Mesh
from jax.sharding import PartitionSpec as P

epsilon = 1e-06
decay_rate = 4.0
half_root = 0.7071067811865476
density_scale = 0.3989422804014327

NY, NX, NC, SECTIONS = 4, 4, 2, 8
DP = ("y", "x", "core")
ROWS = 32
STREAMS = 2
BLOCK = 1024
LIMIT = 16 * 1024 * 1024
bf16 = jnp.bfloat16
f32 = jnp.float32


def params(limit=LIMIT):
    return pltpu.CompilerParams(vmem_limit_bytes=limit, dimension_semantics=("arbitrary",))


def kept_planes(p):
    return (
        p < 3,
        (p == 0) | (p == 3) | (p == 4),
        (p == 1) | (p == 3) | (p == 5),
        (p == 2) | (p >= 4),
    )


def prep_kernel(w_ref, pair_ref, old_ref, left_ref, right_ref, flip_ref, decay_ref, work):
    groups = pair_ref.shape[0]
    lanes = work.shape[0]
    total = jnp.zeros((groups, 128), f32)
    for i in range(lanes):
        cols = slice(i * 128, (i + 1) * 128)
        work[i] = w_ref[:, cols].astype(f32)
        p = pair_ref[:, cols]
        w = [work[i, pl.ds(j, groups, stride=4), :] for j in range(4)]
        v0 = jnp.where(p < 3, w[0], jnp.where(p < 5, w[1], w[2]))
        v1 = jnp.where(p == 0, w[1], jnp.where((p == 1) | (p == 3), w[2], w[3]))
        both = jnp.concatenate([v0, v1], axis=0).astype(bf16)
        if i < lanes // 2:
            left_ref[:, cols] = both
        else:
            right_ref[:, (i - lanes // 2) * 128 : (i - lanes // 2 + 1) * 128] = both
        kept = kept_planes(p)
        old = kept_planes(old_ref[:, cols])
        for j in range(4):
            total = total + jnp.where(kept[j] != old[j], 1.0, 0.0)
            work[i, pl.ds(j, groups, stride=4), :] = jnp.where(kept[j], 0.0, w[j]) * decay_rate
        decay_ref[:, cols] = work[i]
    count = jnp.sum(jnp.sum(total, axis=0, keepdims=True), axis=1, keepdims=True)
    flip_ref[...] = jnp.broadcast_to(count, flip_ref.shape).astype(jnp.int32)


def prep(weight, pairs, earlier):
    rows, width = weight.shape
    groups = rows // 4
    return pl.pallas_call(
        prep_kernel,
        out_shape=[
            jax.ShapeDtypeStruct((2 * groups, width // 2), bf16),
            jax.ShapeDtypeStruct((2 * groups, width // 2), bf16),
            jax.ShapeDtypeStruct((8, 128), jnp.int32),
            jax.ShapeDtypeStruct((rows, width), f32),
        ],
        scratch_shapes=[pltpu.VMEM((width // 128, rows, 128), f32)],
        compiler_params=pltpu.CompilerParams(vmem_limit_bytes=LIMIT),
        name="prep",
    )(weight, pairs, earlier)


def expand_kernel(pos_ref, left_ref, right_ref, pair_ref, old_ref, w_ref, work):
    del pos_ref, old_ref
    lanes = work.shape[0]
    groups = work.shape[1] // 4
    for i in range(lanes):
        cols = slice(i * 128, (i + 1) * 128)
        source = left_ref if i < lanes // 2 else right_ref
        k = i % (lanes // 2)
        both = source[0, 0, :, k * 128 : (k + 1) * 128].astype(f32)
        v0, v1 = both[:groups], both[groups:]
        p = pair_ref[:, cols]
        planes = (
            jnp.where(p < 3, v0, 0.0),
            jnp.where(p == 0, v1, jnp.where((p == 3) | (p == 4), v0, 0.0)),
            jnp.where(p == 5, v0, jnp.where((p == 1) | (p == 3), v1, 0.0)),
            jnp.where((p == 2) | (p >= 4), v1, 0.0),
        )
        for j in range(4):
            work[i, pl.ds(j, groups, stride=4), :] = planes[j]
        w_ref[:, cols] = work[i].astype(bf16)


def expand(pos, left, right, pairs, masked):
    rows, half = left.shape[2:]
    groups = rows // 2
    width = 2 * half

    def left_part(i, pos):
        return (lax.rem(pos[0] - i // NX + NY, NY), lax.rem(pos[1] - lax.rem(i, NX) + NX, NX), 0, 0)

    def right_part(i, pos):
        back_y, back_x, _, _ = left_part(i, pos)
        return (back_x, back_y, 0, 0)

    def block(i, pos):
        return (NC * i + pos[2], 0)

    return pl.pallas_call(
        expand_kernel if masked is not None else (
            lambda pos_ref, left_ref, right_ref, pair_ref, w_ref, work: expand_kernel(
                pos_ref, left_ref, right_ref, pair_ref, None, w_ref, work
            )
        ),
        grid_spec=pltpu.PrefetchScalarGridSpec(
            num_scalar_prefetch=1,
            grid=(NY * NX,),
            in_specs=[
                pl.BlockSpec((1, 1, rows, half), left_part),
                pl.BlockSpec((1, 1, rows, half), right_part),
                pl.BlockSpec((groups, width), block),
            ]
            + ([] if masked is None else [pl.BlockSpec(memory_space=pl.ANY)]),
            out_specs=pl.BlockSpec((4 * groups, width), block),
            scratch_shapes=[pltpu.VMEM((width // 128, 4 * groups, 128), f32)],
        ),
        out_shape=jax.ShapeDtypeStruct((pairs.shape[0] * 4, width), bf16),
        input_output_aliases={} if masked is None else {4: 0},
        compiler_params=params(),
        name="expand",
    )(*((pos, left, right, pairs) + (() if masked is None else (masked,))))


def forward_slot(t, s):
    return t[0] - s[0]


def backward_slot(t, s):
    return t[0] - 2 * SECTIONS + 1 + s[0]


def is_live(j, slots):
    return (j >= 0) & (j < slots)


def forward_kernel(
    slots, t_ref, s_ref, recv_ref, act_ref, gain_ref, w_ref, hb_in, nb_in, db_in,
    out_ref, h_ref, n_ref, d_ref,
):
    del hb_in, nb_in, db_in

    @pl.when(is_live(forward_slot(t_ref, s_ref), slots))
    def _():
        current = jnp.where(s_ref[0] == 0, act_ref[0].astype(f32), recv_ref[...].astype(f32))
        scale = lax.rsqrt(jnp.mean(current * current, axis=-1, keepdims=True) + epsilon)
        h_ref[0] = current.astype(bf16)
        n_ref[0] = (current * scale * gain_ref[...]).astype(bf16)

        def block(n, carry):
            columns = pl.ds(pl.multiple_of(n * BLOCK, BLOCK), BLOCK)
            preact = jnp.dot(n_ref[0], w_ref[:, columns], preferred_element_type=f32)
            cdf = 0.5 * (1.0 + lax.erf(preact * half_root))
            pdf = jnp.exp(-0.5 * preact * preact) * density_scale
            d_ref[0, :, columns] = cdf + preact * pdf
            out_ref[:, columns] = (h_ref[0, :, columns].astype(f32) + preact * cdf).astype(bf16)
            return carry

        lax.fori_loop(0, w_ref.shape[1] // BLOCK, block, 0)


def forward_step(t, s, recv, acts, gain, masked, buffers, slots, first_chunk):
    rows, width = recv.shape
    hb, nb, db = buffers

    def slot(n, t, s):
        j = forward_slot(t, s)
        return (jnp.where(is_live(j, slots), first_chunk + j, STREAMS * slots), 0, 0)

    def chunk(n, t, s):
        return (first_chunk + jnp.clip(forward_slot(t, s), 0, slots - 1), 0, 0)

    whole = lambda n, t, s: (0, 0)
    store = pl.BlockSpec((1, rows, width), slot)
    keep = pl.BlockSpec(memory_space=pl.ANY)
    out, hb, nb, db = pl.pallas_call(
        functools.partial(forward_kernel, slots),
        grid_spec=pltpu.PrefetchScalarGridSpec(
            num_scalar_prefetch=2,
            grid=(1,),
            in_specs=[
                pl.BlockSpec((rows, width), whole),
                pl.BlockSpec((1, rows, width), chunk),
                pl.BlockSpec((1, width), whole),
                pl.BlockSpec(memory_space=pltpu.VMEM),
                keep, keep, keep,
            ],
            out_specs=[pl.BlockSpec((rows, width), whole), store, store, store],
        ),
        out_shape=[
            jax.ShapeDtypeStruct((rows, width), bf16),
            jax.ShapeDtypeStruct(hb.shape, hb.dtype),
            jax.ShapeDtypeStruct(nb.shape, nb.dtype),
            jax.ShapeDtypeStruct(db.shape, db.dtype),
        ],
        input_output_aliases={6: 1, 7: 2, 8: 3},
        compiler_params=params(),
        name="forward",
    )(t, s, recv, acts, gain, masked, hb, nb, db)
    return out, (hb, nb, db)


def backward_kernel(
    slots, t_ref, s_ref, recv_ref, cot_ref, gain_ref, h_ref, d_ref, w_ref, gb_in,
    out_ref, g_ref, up_ref, a_ref,
):
    del gb_in

    @pl.when(is_live(backward_slot(t_ref, s_ref), slots))
    def _():
        upstream = jnp.where(
            s_ref[0] == SECTIONS - 1, cot_ref[0].astype(f32), recv_ref[...].astype(f32)
        )
        up_ref[...] = upstream
        g_ref[0] = (upstream * d_ref[0]).astype(bf16)

        def block(n, carry):
            columns = pl.ds(pl.multiple_of(n * BLOCK, BLOCK), BLOCK)
            grad = lax.dot_general(
                g_ref[0], w_ref[columns, :], (((1,), (1,)), ((), ())), preferred_element_type=f32
            )
            a_ref[:, columns] = grad * gain_ref[:, columns]
            return carry

        lax.fori_loop(0, w_ref.shape[0] // BLOCK, block, 0)
        h = h_ref[0].astype(f32)
        a = a_ref[...]
        scale = lax.rsqrt(jnp.mean(h * h, axis=-1, keepdims=True) + epsilon)
        dot = jnp.mean(a * h, axis=-1, keepdims=True)
        out_ref[...] = (up_ref[...] + scale * a - h * (scale * scale * scale) * dot).astype(bf16)


def backward_step(t, s, recv, cots, gain, masked, buffers, gb, slots, first_chunk):
    rows, width = recv.shape
    hb, _, db = buffers

    def slot(n, t, s):
        j = backward_slot(t, s)
        return (jnp.where(is_live(j, slots), first_chunk + j, STREAMS * slots), 0, 0)

    def chunk(n, t, s):
        return (first_chunk + jnp.clip(backward_slot(t, s), 0, slots - 1), 0, 0)

    whole = lambda n, t, s: (0, 0)
    store = pl.BlockSpec((1, rows, width), slot)
    return pl.pallas_call(
        functools.partial(backward_kernel, slots),
        grid_spec=pltpu.PrefetchScalarGridSpec(
            num_scalar_prefetch=2,
            grid=(1,),
            in_specs=[
                pl.BlockSpec((rows, width), whole),
                pl.BlockSpec((1, rows, width), chunk),
                pl.BlockSpec((1, width), whole),
                store,
                store,
                pl.BlockSpec(memory_space=pltpu.VMEM),
                pl.BlockSpec(memory_space=pl.ANY),
            ],
            out_specs=[pl.BlockSpec((rows, width), whole), store],
            scratch_shapes=[pltpu.VMEM((rows, width), f32), pltpu.VMEM((rows, width), f32)],
        ),
        out_shape=[
            jax.ShapeDtypeStruct((rows, width), bf16),
            jax.ShapeDtypeStruct(gb.shape, gb.dtype),
        ],
        input_output_aliases={8: 1},
        compiler_params=params(),
        name="backward",
    )(t, s, recv, cots, gain, hb, db, masked, gb)


def ring(x, axis, distance):
    n = lax.axis_size(axis)
    return lax.ppermute(x, axis, [(i, (i + distance) % n) for i in range(n)])


def gather4_direct(block, axis):
    return jnp.stack([block, ring(block, axis, 1), ring(block, axis, 2), ring(block, axis, -1)])


def gather4_near(block, axis):
    half = block.shape[0] // 2
    top, bottom = block[:half], block[half:]
    back_top = ring(top, axis, 1)
    ahead_bottom = ring(bottom, axis, -1)
    return back_top, ahead_bottom, ring(bottom, axis, 1), ring(top, axis, -1)


def gather4_join(block, near, far):
    back_top, ahead_bottom, back_bottom, ahead_top = near
    join = lambda a, b: jnp.concatenate([a, b], axis=0)
    return jnp.stack([block, join(back_top, back_bottom), join(*far), join(ahead_top, ahead_bottom)])


def add(*terms):
    total = terms[0].astype(f32)
    for term in terms[1:]:
        total = total + term.astype(f32)
    return total


def scatter4(chunks, me, axis, dim):
    own, nxt, across, prev = [
        lax.dynamic_index_in_dim(chunks, lax.rem(me + k, 4), dim, keepdims=False) for k in range(4)
    ]
    return add(own, ring(nxt, axis, 1), ring(prev, axis, -1), ring(across, axis, 2))


def scatter4_relay(chunks, me, axis, dim):
    own, nxt, across, prev = [
        lax.dynamic_index_in_dim(chunks, lax.rem(me + k, 4), dim, keepdims=False) for k in range(4)
    ]
    half = own.shape[0] // 2
    forth = ring(across[:half], axis, 1)
    back = ring(across[half:], axis, -1)
    nxt_rest = ring(nxt[half:], axis, 1)
    prev_rest = ring(prev[:half], axis, -1)
    nxt_sum = ring(add(nxt[:half], forth).astype(bf16), axis, 1)
    prev_sum = ring(add(prev[half:], back).astype(bf16), axis, -1)
    return (add(own[:half], nxt_sum, prev_rest), add(own[half:], nxt_rest, prev_sum))


def token_product(x, g):
    return lax.dot_general(x, g, (((0,), (0,)), ((), ())), preferred_element_type=f32)


def body(activations, cotangent, weight, norm_gain, pair_mask, earlier_mask):
    section = lax.axis_index("section")
    y, x, core = (lax.axis_index(name) for name in DP)
    replica = (y * NX + x) * NC + core
    micro_count, row_count, width = activations.shape
    tokens = micro_count * row_count
    chunks = tokens // ROWS
    slots = chunks // STREAMS
    acts = activations.reshape(chunks, ROWS, width)
    cots = cotangent.reshape(chunks, ROWS, width)
    s = section.reshape(1).astype(jnp.int32)
    half = width // 2

    own_groups = earlier_mask.shape[1]
    own_pairs = lax.dynamic_slice_in_dim(pair_mask[0], replica * own_groups, own_groups, 0)
    left, right, flips, decay = prep(weight[0], own_pairs, earlier_mask[0])

    left = gather4_direct(left, "x")
    right = gather4_direct(right, "y")
    count = flips + ring(flips, "core", 1)
    left, right, count = lax.optimization_barrier((left, right, count))
    rows = left.shape[1]
    left, right = left.reshape(4 * rows, half), right.reshape(4 * rows, half)
    left_near, right_near = gather4_near(left, "y"), gather4_near(right, "x")
    counts = gather4_direct(count, "x")
    left_far = ring(left_near[0], "y", 1), ring(left_near[1], "y", -1)
    right_far = ring(right_near[0], "x", 1), ring(right_near[1], "x", -1)
    left_far, right_far, counts = lax.optimization_barrier((left_far, right_far, counts))
    counts = gather4_direct(counts.sum(axis=0), "y")
    right = gather4_join(right, right_near, right_far).reshape(4, 4, rows, half)
    right_other = ring(right, "core", 1)
    left = gather4_join(left, left_near, left_far).reshape(4, 4, rows, half)
    left_other = ring(left, "core", 1)
    pos = jnp.stack([y, x, core]).astype(jnp.int32)
    pos_other = jnp.stack([y, x, 1 - core]).astype(jnp.int32)
    pairs_hbm = pltpu.with_memory_space_constraint(pair_mask[0], pltpu.HBM)
    masked = expand(pos, left, right, pairs_hbm, None)
    left_other, right_other, counts = lax.optimization_barrier((left_other, right_other, counts))
    count = counts.sum(axis=0)
    masked = expand(pos_other, left_other, right_other, pairs_hbm, masked)

    fwd_ticks = slots + SECTIONS - 1
    zero = lambda dtype: jnp.zeros((chunks + 1, ROWS, width), dtype)
    buffers = (zero(bf16), zero(bf16), zero(f32))
    grads = zero(bf16)
    fwd = [acts[0] for _ in range(STREAMS)]
    bwd = [cots[0] for _ in range(STREAMS)]
    for tick in range(SECTIONS + fwd_ticks):
        now = jnp.full((1,), tick, jnp.int32)
        for k in range(STREAMS):
            if tick >= SECTIONS:
                out, grads = backward_step(
                    now, s, bwd[k], cots, norm_gain, masked, buffers, grads, slots, k * slots
                )
                if tick < SECTIONS + fwd_ticks - 1:
                    bwd[k] = ring(out, "section", -1)
            if tick < fwd_ticks:
                out, buffers = forward_step(
                    now, s, fwd[k], acts, norm_gain, masked, buffers, slots, k * slots
                )
                if tick < fwd_ticks - 1:
                    fwd[k] = ring(out, "section", 1)

    grads, core, y, x = lax.optimization_barrier((grads, core, y, x))
    normed = buffers[1][:chunks].reshape(tokens, width)
    grad = grads[:chunks].reshape(tokens, width)
    g_left, g_right = grad[:, :half], grad[:, half:]
    first = core == 0
    g_mine = jnp.where(first, g_left, g_right)
    normed_other = ring(normed, "core", 1)
    g_other = ring(jnp.where(first, g_right, g_left), "core", 1)
    quarter = half // 2
    parts = []
    for c in range(2):
        cols = slice(c * quarter, (c + 1) * quarter)
        partial = token_product(normed, g_mine[:, cols]) + token_product(normed_other, g_other[:, cols])
        parts.append(partial.astype(bf16).reshape(NY, NX, 2 * row_count, quarter))
    part_l = jnp.concatenate(scatter4_relay(parts[0], x, "x", 1), axis=0).astype(bf16)
    part_r = jnp.concatenate(scatter4_relay(parts[1], y, "y", 0), axis=0).astype(bf16)
    part_l = scatter4(part_l, y, "y", 0)
    part_r = scatter4(part_r, x, "x", 0)
    mine = jnp.concatenate([part_l, part_r], axis=1)
    top, bottom = mine[:row_count], mine[row_count:]
    own = jnp.where(first, top, bottom)
    other = ring(jnp.where(first, bottom, top).astype(bf16), "core", 1).astype(f32)
    total = jnp.where(
        first, jnp.concatenate([own, other], axis=1), jnp.concatenate([other, own], axis=1)
    )
    gradient = total / math.sqrt(tokens * NY * NX * NC) + decay

    return gradient[None], count[0, :1]


def solution(mesh):
    cube = Mesh(mesh.devices.reshape(NY, NX, NC, SECTIONS), (*DP, "section"))
    placed = (
        P(None, DP, None),
        P(None, DP, None),
        P("section", DP, None),
        P("section", None),
        P("section", None, None),
        P("section", DP, None),
    )
    return jax.shard_map(
        body,
        mesh=cube,
        in_specs=placed,
        out_specs=(P("section", DP, None), P("section")),
        check_vma=False,
    )
```

```python
import functools
import math

import jax
import jax.numpy as jnp
from jax import lax
from jax.experimental import pallas as pl
from jax.experimental.pallas import tpu as pltpu
from jax.sharding import Mesh
from jax.sharding import PartitionSpec as P

epsilon = 1e-06
decay_rate = 4.0
half_root = 0.7071067811865476
density_scale = 0.3989422804014327

NY, NX, NC, SECTIONS = 4, 4, 2, 8
DP = ("y", "x", "core")
ROWS = 32
STREAMS = 2
BLOCK = 1024
LIMIT = 16 * 1024 * 1024
bf16 = jnp.bfloat16
f32 = jnp.float32


def params(limit=LIMIT):
    return pltpu.CompilerParams(vmem_limit_bytes=limit, dimension_semantics=("arbitrary",))


def kept_planes(p):
    return (
        p < 3,
        (p == 0) | (p == 3) | (p == 4),
        (p == 1) | (p == 3) | (p == 5),
        (p == 2) | (p >= 4),
    )


def prep_kernel(w_ref, pair_ref, old_ref, left_ref, right_ref, flip_ref, decay_ref, work):
    groups = pair_ref.shape[0]
    lanes = work.shape[0]
    total = jnp.zeros((groups, 128), f32)
    for i in range(lanes):
        cols = slice(i * 128, (i + 1) * 128)
        work[i] = w_ref[:, cols].astype(f32)
        p = pair_ref[:, cols]
        w = [work[i, pl.ds(j, groups, stride=4), :] for j in range(4)]
        v0 = jnp.where(p < 3, w[0], jnp.where(p < 5, w[1], w[2]))
        v1 = jnp.where(p == 0, w[1], jnp.where((p == 1) | (p == 3), w[2], w[3]))
        both = jnp.concatenate([v0, v1], axis=0).astype(bf16)
        if i < lanes // 2:
            left_ref[:, cols] = both
        else:
            right_ref[:, (i - lanes // 2) * 128 : (i - lanes // 2 + 1) * 128] = both
        kept = kept_planes(p)
        old = kept_planes(old_ref[:, cols])
        for j in range(4):
            total = total + jnp.where(kept[j] != old[j], 1.0, 0.0)
            work[i, pl.ds(j, groups, stride=4), :] = jnp.where(kept[j], 0.0, w[j]) * decay_rate
        decay_ref[:, cols] = work[i]
    count = jnp.sum(jnp.sum(total, axis=0, keepdims=True), axis=1, keepdims=True)
    flip_ref[...] = jnp.broadcast_to(count, flip_ref.shape).astype(jnp.int32)


def prep(weight, pairs, earlier):
    rows, width = weight.shape
    groups = rows // 4
    return pl.pallas_call(
        prep_kernel,
        out_shape=[
            jax.ShapeDtypeStruct((2 * groups, width // 2), bf16),
            jax.ShapeDtypeStruct((2 * groups, width // 2), bf16),
            jax.ShapeDtypeStruct((8, 128), jnp.int32),
            jax.ShapeDtypeStruct((rows, width), f32),
        ],
        scratch_shapes=[pltpu.VMEM((width // 128, rows, 128), f32)],
        compiler_params=pltpu.CompilerParams(vmem_limit_bytes=LIMIT),
        name="prep",
    )(weight, pairs, earlier)


def expand_kernel(pos_ref, lo_ref, ro_ref, lt_ref, rt_ref, pair_ref, w_ref, work):
    groups = lo_ref.shape[2] // 2
    half = lo_ref.shape[3]
    me_y, me_x, core = pos_ref[0], pos_ref[1], pos_ref[2]
    back_y = lax.rem(me_y - pl.program_id(0) + NY, NY)

    def chip(x, carry):
        back_x = lax.rem(me_x - x + NX, NX)
        for c, left_ref, right_ref in ((core, lo_ref, ro_ref), (1 - core, lt_ref, rt_ref)):
            here = x * NC + c
            rows = pl.ds(pl.multiple_of(here * groups, groups), groups)
            out = pl.ds(pl.multiple_of(here * 4 * groups, 4 * groups), 4 * groups)
            for i in range(2 * half // 128):
                cols = slice(i * 128, (i + 1) * 128)
                if i < half // 128:
                    both = left_ref[back_y, back_x, :, cols].astype(f32)
                else:
                    both = right_ref[back_x, back_y, :, i * 128 - half : (i + 1) * 128 - half].astype(f32)
                v0, v1 = both[:groups], both[groups:]
                p = pair_ref[rows, cols]
                planes = (
                    jnp.where(p < 3, v0, 0.0),
                    jnp.where(p == 0, v1, jnp.where((p == 3) | (p == 4), v0, 0.0)),
                    jnp.where(p == 5, v0, jnp.where((p == 1) | (p == 3), v1, 0.0)),
                    jnp.where((p == 2) | (p >= 4), v1, 0.0),
                )
                for j in range(4):
                    work[i, pl.ds(j, groups, stride=4), :] = planes[j]
                w_ref[out, cols] = work[i].astype(bf16)
        return carry

    lax.fori_loop(0, NX, chip, 0)


def expand(pos, left_own, right_own, left_other, right_other, pairs):
    rows, half = left_own.shape[2:]
    groups = rows // 2
    width = 2 * half
    step = pairs.shape[0] // NY
    whole = pl.BlockSpec(memory_space=pltpu.VMEM)
    return pl.pallas_call(
        expand_kernel,
        grid_spec=pltpu.PrefetchScalarGridSpec(
            num_scalar_prefetch=1,
            grid=(NY,),
            in_specs=[whole] * 4 + [pl.BlockSpec((step, width), lambda i, pos: (i, 0))],
            out_specs=pl.BlockSpec((4 * step, width), lambda i, pos: (i, 0)),
            scratch_shapes=[pltpu.VMEM((width // 128, 4 * groups, 128), f32)],
        ),
        out_shape=jax.ShapeDtypeStruct((4 * pairs.shape[0], width), bf16),
        compiler_params=params(),
        name="expand",
    )(pos, left_own, right_own, left_other, right_other, pairs)


def forward_slot(t, s):
    return t[0] - s[0]


def backward_slot(t, s):
    return t[0] - 2 * SECTIONS + 1 + s[0]


def is_live(j, slots):
    return (j >= 0) & (j < slots)


def forward_kernel(
    slots, t_ref, s_ref, recv_ref, act_ref, gain_ref, w_ref, hb_in, nb_in, db_in,
    out_ref, h_ref, n_ref, d_ref,
):
    del hb_in, nb_in, db_in

    @pl.when(is_live(forward_slot(t_ref, s_ref), slots))
    def _():
        current = jnp.where(s_ref[0] == 0, act_ref[0].astype(f32), recv_ref[...].astype(f32))
        scale = lax.rsqrt(jnp.mean(current * current, axis=-1, keepdims=True) + epsilon)
        h_ref[0] = current.astype(bf16)
        n_ref[0] = (current * scale * gain_ref[...]).astype(bf16)

        def block(n, carry):
            columns = pl.ds(pl.multiple_of(n * BLOCK, BLOCK), BLOCK)
            preact = jnp.dot(n_ref[0], w_ref[:, columns], preferred_element_type=f32)
            cdf = 0.5 * (1.0 + lax.erf(preact * half_root))
            pdf = jnp.exp(-0.5 * preact * preact) * density_scale
            d_ref[0, :, columns] = cdf + preact * pdf
            out_ref[:, columns] = (h_ref[0, :, columns].astype(f32) + preact * cdf).astype(bf16)
            return carry

        lax.fori_loop(0, w_ref.shape[1] // BLOCK, block, 0)


def forward_step(t, s, recv, acts, gain, masked, buffers, slots, first_chunk):
    rows, width = recv.shape
    hb, nb, db = buffers

    def slot(n, t, s):
        j = forward_slot(t, s)
        return (jnp.where(is_live(j, slots), first_chunk + j, STREAMS * slots), 0, 0)

    def chunk(n, t, s):
        return (first_chunk + jnp.clip(forward_slot(t, s), 0, slots - 1), 0, 0)

    whole = lambda n, t, s: (0, 0)
    store = pl.BlockSpec((1, rows, width), slot)
    keep = pl.BlockSpec(memory_space=pl.ANY)
    out, hb, nb, db = pl.pallas_call(
        functools.partial(forward_kernel, slots),
        grid_spec=pltpu.PrefetchScalarGridSpec(
            num_scalar_prefetch=2,
            grid=(1,),
            in_specs=[
                pl.BlockSpec((rows, width), whole),
                pl.BlockSpec((1, rows, width), chunk),
                pl.BlockSpec((1, width), whole),
                pl.BlockSpec(memory_space=pltpu.VMEM),
                keep, keep, keep,
            ],
            out_specs=[pl.BlockSpec((rows, width), whole), store, store, store],
        ),
        out_shape=[
            jax.ShapeDtypeStruct((rows, width), bf16),
            jax.ShapeDtypeStruct(hb.shape, hb.dtype),
            jax.ShapeDtypeStruct(nb.shape, nb.dtype),
            jax.ShapeDtypeStruct(db.shape, db.dtype),
        ],
        input_output_aliases={6: 1, 7: 2, 8: 3},
        compiler_params=params(),
        name="forward",
    )(t, s, recv, acts, gain, masked, hb, nb, db)
    return out, (hb, nb, db)


def backward_kernel(
    slots, t_ref, s_ref, recv_ref, cot_ref, gain_ref, h_ref, d_ref, w_ref, gb_in,
    out_ref, g_ref, up_ref, a_ref,
):
    del gb_in

    @pl.when(is_live(backward_slot(t_ref, s_ref), slots))
    def _():
        upstream = jnp.where(
            s_ref[0] == SECTIONS - 1, cot_ref[0].astype(f32), recv_ref[...].astype(f32)
        )
        up_ref[...] = upstream
        g_ref[0] = (upstream * d_ref[0]).astype(bf16)

        def block(n, carry):
            columns = pl.ds(pl.multiple_of(n * BLOCK, BLOCK), BLOCK)
            grad = lax.dot_general(
                g_ref[0], w_ref[columns, :], (((1,), (1,)), ((), ())), preferred_element_type=f32
            )
            a_ref[:, columns] = grad * gain_ref[:, columns]
            return carry

        lax.fori_loop(0, w_ref.shape[0] // BLOCK, block, 0)
        h = h_ref[0].astype(f32)
        a = a_ref[...]
        scale = lax.rsqrt(jnp.mean(h * h, axis=-1, keepdims=True) + epsilon)
        dot = jnp.mean(a * h, axis=-1, keepdims=True)
        out_ref[...] = (up_ref[...] + scale * a - h * (scale * scale * scale) * dot).astype(bf16)


def backward_step(t, s, recv, cots, gain, masked, buffers, gb, slots, first_chunk):
    rows, width = recv.shape
    hb, _, db = buffers

    def slot(n, t, s):
        j = backward_slot(t, s)
        return (jnp.where(is_live(j, slots), first_chunk + j, STREAMS * slots), 0, 0)

    def chunk(n, t, s):
        return (first_chunk + jnp.clip(backward_slot(t, s), 0, slots - 1), 0, 0)

    whole = lambda n, t, s: (0, 0)
    store = pl.BlockSpec((1, rows, width), slot)
    return pl.pallas_call(
        functools.partial(backward_kernel, slots),
        grid_spec=pltpu.PrefetchScalarGridSpec(
            num_scalar_prefetch=2,
            grid=(1,),
            in_specs=[
                pl.BlockSpec((rows, width), whole),
                pl.BlockSpec((1, rows, width), chunk),
                pl.BlockSpec((1, width), whole),
                store,
                store,
                pl.BlockSpec(memory_space=pltpu.VMEM),
                pl.BlockSpec(memory_space=pl.ANY),
            ],
            out_specs=[pl.BlockSpec((rows, width), whole), store],
            scratch_shapes=[pltpu.VMEM((rows, width), f32), pltpu.VMEM((rows, width), f32)],
        ),
        out_shape=[
            jax.ShapeDtypeStruct((rows, width), bf16),
            jax.ShapeDtypeStruct(gb.shape, gb.dtype),
        ],
        input_output_aliases={8: 1},
        compiler_params=params(),
        name="backward",
    )(t, s, recv, cots, gain, hb, db, masked, gb)


def ring(x, axis, distance):
    n = lax.axis_size(axis)
    return lax.ppermute(x, axis, [(i, (i + distance) % n) for i in range(n)])


def gather4(block, axis, direct):
    back = ring(block, axis, 1)
    ahead = ring(block, axis, -1)
    if direct:
        across = ring(block, axis, 2)
    else:
        half = block.shape[0] // 2
        across = jnp.concatenate([ring(back[:half], axis, 1), ring(ahead[half:], axis, -1)], axis=0)
    return jnp.stack([block, back, across, ahead])


def add(*terms):
    total = terms[0].astype(f32)
    for term in terms[1:]:
        total = total + term.astype(f32)
    return total


def scatter4(chunks, me, axis, dim):
    own, nxt, across, prev = [
        lax.dynamic_index_in_dim(chunks, lax.rem(me + k, 4), dim, keepdims=False) for k in range(4)
    ]
    return add(own, ring(nxt, axis, 1), ring(prev, axis, -1), ring(across, axis, 2))


def pairwise(x, axis, bit):
    n = lax.axis_size(axis)
    return x + lax.ppermute(x, axis, [(i, i ^ bit) for i in range(n)])


def token_product(x, g):
    return lax.dot_general(x, g, (((0,), (0,)), ((), ())), preferred_element_type=f32)


def body(activations, cotangent, weight, norm_gain, pair_mask, earlier_mask):
    section = lax.axis_index("section")
    y, x, core = (lax.axis_index(name) for name in DP)
    replica = (y * NX + x) * NC + core
    micro_count, row_count, width = activations.shape
    tokens = micro_count * row_count
    chunks = tokens // ROWS
    slots = chunks // STREAMS
    acts = activations.reshape(chunks, ROWS, width)
    cots = cotangent.reshape(chunks, ROWS, width)
    s = section.reshape(1).astype(jnp.int32)
    half = width // 2

    own_groups = earlier_mask.shape[1]
    own_pairs = lax.dynamic_slice_in_dim(pair_mask[0], replica * own_groups, own_groups, 0)
    left, right, flips, decay = prep(weight[0], own_pairs, earlier_mask[0])

    left = gather4(left, "x", True)
    right = gather4(right, "y", True)
    rows = left.shape[1]
    right = gather4(right.reshape(4 * rows, half), "x", False).reshape(4, 4, rows, half)
    left = gather4(left.reshape(4 * rows, half), "y", False).reshape(4, 4, rows, half)
    right_other = ring(right, "core", 1)
    left_other = ring(left, "core", 1)
    pos = jnp.stack([y, x, core]).astype(jnp.int32)
    pairs_hbm = pltpu.with_memory_space_constraint(pair_mask[0], pltpu.HBM)
    masked = expand(pos, left, right, left_other, right_other, pairs_hbm)

    fwd_ticks = slots + SECTIONS - 1
    zero = lambda dtype: jnp.zeros((chunks + 1, ROWS, width), dtype)
    buffers = (zero(bf16), zero(bf16), zero(f32))
    grads = zero(bf16)
    fwd = [acts[0] for _ in range(STREAMS)]
    bwd = [cots[0] for _ in range(STREAMS)]
    for tick in range(SECTIONS + fwd_ticks):
        now = jnp.full((1,), tick, jnp.int32)
        for k in range(STREAMS):
            if tick >= SECTIONS:
                out, grads = backward_step(
                    now, s, bwd[k], cots, norm_gain, masked, buffers, grads, slots, k * slots
                )
                if tick < SECTIONS + fwd_ticks - 1:
                    bwd[k] = ring(out, "section", -1)
            if tick < fwd_ticks:
                out, buffers = forward_step(
                    now, s, fwd[k], acts, norm_gain, masked, buffers, slots, k * slots
                )
                if tick < fwd_ticks - 1:
                    fwd[k] = ring(out, "section", 1)

    grads, core, y, x = lax.optimization_barrier((grads, core, y, x))
    normed = buffers[1][:chunks].reshape(tokens, width)
    grad = grads[:chunks].reshape(tokens, width)
    g_left, g_right = grad[:, :half], grad[:, half:]
    first = core == 0
    g_mine = jnp.where(first, g_left, g_right)
    normed_other = ring(normed, "core", 1)
    g_other = ring(jnp.where(first, g_right, g_left), "core", 1)
    quarter = half // 2
    parts = []
    for c in range(2):
        cols = slice(c * quarter, (c + 1) * quarter)
        partial = token_product(normed, g_mine[:, cols]) + token_product(normed_other, g_other[:, cols])
        parts.append(partial.astype(bf16).reshape(NY, NX, 2 * row_count, quarter))
    part_l = scatter4(parts[0], x, "x", 1).astype(bf16)
    part_r = scatter4(parts[1], y, "y", 0).astype(bf16)
    part_l = scatter4(part_l, y, "y", 0)
    part_r = scatter4(part_r, x, "x", 0)
    mine = jnp.concatenate([part_l, part_r], axis=1)
    top, bottom = mine[:row_count], mine[row_count:]
    own = jnp.where(first, top, bottom)
    other = ring(jnp.where(first, bottom, top).astype(bf16), "core", 1).astype(f32)
    total = jnp.where(
        first, jnp.concatenate([own, other], axis=1), jnp.concatenate([other, own], axis=1)
    )
    gradient = total / math.sqrt(tokens * NY * NX * NC) + decay

    count = pairwise(pairwise(pairwise(flips, "core", 1), "x", 1), "x", 2)
    count = pairwise(pairwise(count, "y", 1), "y", 2)
    return gradient[None], count[0, :1]


def solution(mesh):
    cube = Mesh(mesh.devices.reshape(NY, NX, NC, SECTIONS), (*DP, "section"))
    placed = (
        P(None, DP, None),
        P(None, DP, None),
        P("section", DP, None),
        P("section", None),
        P("section", None, None),
        P("section", DP, None),
    )
    return jax.shard_map(
        body,
        mesh=cube,
        in_specs=placed,
        out_specs=(P("section", DP, None), P("section")),
        check_vma=False,
    )
```

```python
import functools
import math

import jax
import jax.numpy as jnp
from jax import lax
from jax.experimental import pallas as pl
from jax.experimental.pallas import tpu as pltpu
from jax.sharding import Mesh
from jax.sharding import PartitionSpec as P

epsilon = 1e-06
decay_rate = 4.0
half_root = 0.7071067811865476
density_scale = 0.3989422804014327

NY, NX, NC, SECTIONS = 4, 4, 2, 8
DP = ("y", "x", "core")
ROWS = 32
STREAMS = 2
BLOCK = 1024
LIMIT = 16 * 1024 * 1024
bf16 = jnp.bfloat16
f32 = jnp.float32


def params(limit=LIMIT):
    return pltpu.CompilerParams(vmem_limit_bytes=limit, dimension_semantics=("arbitrary",))


def kept_planes(p):
    return (
        p < 3,
        (p == 0) | (p == 3) | (p == 4),
        (p == 1) | (p == 3) | (p == 5),
        (p == 2) | (p >= 4),
    )


def prep_kernel(rep_ref, w_ref, pair_ref, old_ref, left_ref, right_ref, flip_ref, decay_ref, work):
    del rep_ref
    groups = pair_ref.shape[0]
    lanes = work.shape[0]
    total = jnp.zeros((groups, 128), f32)
    for i in range(lanes):
        cols = slice(i * 128, (i + 1) * 128)
        work[i] = w_ref[:, cols].astype(f32)
        p = pair_ref[:, cols]
        w = [work[i, pl.ds(j, groups, stride=4), :] for j in range(4)]
        v0 = jnp.where(p < 3, w[0], jnp.where(p < 5, w[1], w[2]))
        v1 = jnp.where(p == 0, w[1], jnp.where((p == 1) | (p == 3), w[2], w[3]))
        both = jnp.concatenate([v0, v1], axis=0).astype(bf16)
        if i < lanes // 2:
            left_ref[:, cols] = both
        else:
            right_ref[:, (i - lanes // 2) * 128 : (i - lanes // 2 + 1) * 128] = both
        kept = kept_planes(p)
        old = kept_planes(old_ref[:, cols])
        for j in range(4):
            total = total + jnp.where(kept[j] != old[j], 1.0, 0.0)
            work[i, pl.ds(j, groups, stride=4), :] = jnp.where(kept[j], 0.0, w[j]) * decay_rate
        decay_ref[:, cols] = work[i]
    count = jnp.sum(jnp.sum(total, axis=0, keepdims=True), axis=1, keepdims=True)
    flip_ref[...] = jnp.broadcast_to(count, flip_ref.shape).astype(jnp.int32)


def prep(replica, weight, pairs, earlier):
    rows, width = weight.shape
    groups = rows // 4
    whole = lambda i, r: (0, 0)
    return pl.pallas_call(
        prep_kernel,
        grid_spec=pltpu.PrefetchScalarGridSpec(
            num_scalar_prefetch=1,
            grid=(1,),
            in_specs=[
                pl.BlockSpec((rows, width), whole),
                pl.BlockSpec((groups, width), lambda i, r: (r[0], 0)),
                pl.BlockSpec((groups, width), whole),
            ],
            out_specs=[
                pl.BlockSpec((2 * groups, width // 2), whole),
                pl.BlockSpec((2 * groups, width // 2), whole),
                pl.BlockSpec((8, 128), whole),
                pl.BlockSpec((rows, width), whole),
            ],
            scratch_shapes=[pltpu.VMEM((width // 128, rows, 128), f32)],
        ),
        out_shape=[
            jax.ShapeDtypeStruct((2 * groups, width // 2), bf16),
            jax.ShapeDtypeStruct((2 * groups, width // 2), bf16),
            jax.ShapeDtypeStruct((8, 128), jnp.int32),
            jax.ShapeDtypeStruct((rows, width), f32),
        ],
        compiler_params=params(),
        name="prep",
    )(replica, weight, pairs, earlier)


def expand_kernel(pos_ref, lo_ref, ro_ref, lt_ref, rt_ref, pair_ref, w_ref, work):
    groups = lo_ref.shape[2] // 2
    half = lo_ref.shape[3]
    me_y, me_x, core = pos_ref[0], pos_ref[1], pos_ref[2]
    back_y = lax.rem(me_y - pl.program_id(0) + NY, NY)

    def chip(x, carry):
        back_x = lax.rem(me_x - x + NX, NX)
        for c, left_ref, right_ref in ((core, lo_ref, ro_ref), (1 - core, lt_ref, rt_ref)):
            here = x * NC + c
            rows = pl.ds(pl.multiple_of(here * groups, groups), groups)
            out = pl.ds(pl.multiple_of(here * 4 * groups, 4 * groups), 4 * groups)
            for i in range(2 * half // 128):
                cols = slice(i * 128, (i + 1) * 128)
                if i < half // 128:
                    both = left_ref[back_y, back_x, :, cols].astype(f32)
                else:
                    both = right_ref[back_x, back_y, :, i * 128 - half : (i + 1) * 128 - half].astype(f32)
                v0, v1 = both[:groups], both[groups:]
                p = pair_ref[rows, cols]
                planes = (
                    jnp.where(p < 3, v0, 0.0),
                    jnp.where(p == 0, v1, jnp.where((p == 3) | (p == 4), v0, 0.0)),
                    jnp.where(p == 5, v0, jnp.where((p == 1) | (p == 3), v1, 0.0)),
                    jnp.where((p == 2) | (p >= 4), v1, 0.0),
                )
                for j in range(4):
                    work[i, pl.ds(j, groups, stride=4), :] = planes[j]
                w_ref[out, cols] = work[i].astype(bf16)
        return carry

    lax.fori_loop(0, NX, chip, 0)


def expand(pos, left_own, right_own, left_other, right_other, pairs):
    rows, half = left_own.shape[2:]
    groups = rows // 2
    width = 2 * half
    step = pairs.shape[0] // NY
    whole = pl.BlockSpec(memory_space=pltpu.VMEM)
    return pl.pallas_call(
        expand_kernel,
        grid_spec=pltpu.PrefetchScalarGridSpec(
            num_scalar_prefetch=1,
            grid=(NY,),
            in_specs=[whole] * 4 + [pl.BlockSpec((step, width), lambda i, pos: (i, 0))],
            out_specs=pl.BlockSpec((4 * step, width), lambda i, pos: (i, 0)),
            scratch_shapes=[pltpu.VMEM((width // 128, 4 * groups, 128), f32)],
        ),
        out_shape=jax.ShapeDtypeStruct((4 * pairs.shape[0], width), bf16),
        compiler_params=params(),
        name="expand",
    )(pos, left_own, right_own, left_other, right_other, pairs)


def forward_slot(t, s):
    return t[0] - s[0]


def backward_slot(t, s):
    return t[0] - 2 * SECTIONS + 1 + s[0]


def is_live(j, slots):
    return (j >= 0) & (j < slots)


def forward_kernel(
    slots, t_ref, s_ref, recv_ref, act_ref, gain_ref, w_ref, hb_in, nb_in, db_in,
    out_ref, h_ref, n_ref, d_ref,
):
    del hb_in, nb_in, db_in

    @pl.when(is_live(forward_slot(t_ref, s_ref), slots))
    def _():
        current = jnp.where(s_ref[0] == 0, act_ref[0].astype(f32), recv_ref[...].astype(f32))
        scale = lax.rsqrt(jnp.mean(current * current, axis=-1, keepdims=True) + epsilon)
        h_ref[0] = current.astype(bf16)
        n_ref[0] = (current * scale * gain_ref[...]).astype(bf16)

        def block(n, carry):
            columns = pl.ds(pl.multiple_of(n * BLOCK, BLOCK), BLOCK)
            preact = jnp.dot(n_ref[0], w_ref[:, columns], preferred_element_type=f32)
            cdf = 0.5 * (1.0 + lax.erf(preact * half_root))
            pdf = jnp.exp(-0.5 * preact * preact) * density_scale
            d_ref[0, :, columns] = cdf + preact * pdf
            out_ref[:, columns] = (h_ref[0, :, columns].astype(f32) + preact * cdf).astype(bf16)
            return carry

        lax.fori_loop(0, w_ref.shape[1] // BLOCK, block, 0)


def forward_step(t, s, recv, acts, gain, masked, buffers, slots, first_chunk):
    rows, width = recv.shape
    hb, nb, db = buffers

    def slot(n, t, s):
        j = forward_slot(t, s)
        return (jnp.where(is_live(j, slots), first_chunk + j, STREAMS * slots), 0, 0)

    def chunk(n, t, s):
        return (first_chunk + jnp.clip(forward_slot(t, s), 0, slots - 1), 0, 0)

    whole = lambda n, t, s: (0, 0)
    store = pl.BlockSpec((1, rows, width), slot)
    keep = pl.BlockSpec(memory_space=pl.ANY)
    out, hb, nb, db = pl.pallas_call(
        functools.partial(forward_kernel, slots),
        grid_spec=pltpu.PrefetchScalarGridSpec(
            num_scalar_prefetch=2,
            grid=(1,),
            in_specs=[
                pl.BlockSpec((rows, width), whole),
                pl.BlockSpec((1, rows, width), chunk),
                pl.BlockSpec((1, width), whole),
                pl.BlockSpec(memory_space=pltpu.VMEM),
                keep, keep, keep,
            ],
            out_specs=[pl.BlockSpec((rows, width), whole), store, store, store],
        ),
        out_shape=[
            jax.ShapeDtypeStruct((rows, width), bf16),
            jax.ShapeDtypeStruct(hb.shape, hb.dtype),
            jax.ShapeDtypeStruct(nb.shape, nb.dtype),
            jax.ShapeDtypeStruct(db.shape, db.dtype),
        ],
        input_output_aliases={6: 1, 7: 2, 8: 3},
        compiler_params=params(),
        name="forward",
    )(t, s, recv, acts, gain, masked, hb, nb, db)
    return out, (hb, nb, db)


def backward_kernel(
    slots, t_ref, s_ref, recv_ref, cot_ref, gain_ref, h_ref, d_ref, w_ref, gb_in,
    out_ref, g_ref, up_ref, a_ref,
):
    del gb_in

    @pl.when(is_live(backward_slot(t_ref, s_ref), slots))
    def _():
        upstream = jnp.where(
            s_ref[0] == SECTIONS - 1, cot_ref[0].astype(f32), recv_ref[...].astype(f32)
        )
        up_ref[...] = upstream
        g_ref[0] = (upstream * d_ref[0]).astype(bf16)

        def block(n, carry):
            columns = pl.ds(pl.multiple_of(n * BLOCK, BLOCK), BLOCK)
            grad = lax.dot_general(
                g_ref[0], w_ref[columns, :], (((1,), (1,)), ((), ())), preferred_element_type=f32
            )
            a_ref[:, columns] = grad * gain_ref[:, columns]
            return carry

        lax.fori_loop(0, w_ref.shape[0] // BLOCK, block, 0)
        h = h_ref[0].astype(f32)
        a = a_ref[...]
        scale = lax.rsqrt(jnp.mean(h * h, axis=-1, keepdims=True) + epsilon)
        dot = jnp.mean(a * h, axis=-1, keepdims=True)
        out_ref[...] = (up_ref[...] + scale * a - h * (scale * scale * scale) * dot).astype(bf16)


def backward_step(t, s, recv, cots, gain, masked, buffers, gb, slots, first_chunk):
    rows, width = recv.shape
    hb, _, db = buffers

    def slot(n, t, s):
        j = backward_slot(t, s)
        return (jnp.where(is_live(j, slots), first_chunk + j, STREAMS * slots), 0, 0)

    def chunk(n, t, s):
        return (first_chunk + jnp.clip(backward_slot(t, s), 0, slots - 1), 0, 0)

    whole = lambda n, t, s: (0, 0)
    store = pl.BlockSpec((1, rows, width), slot)
    return pl.pallas_call(
        functools.partial(backward_kernel, slots),
        grid_spec=pltpu.PrefetchScalarGridSpec(
            num_scalar_prefetch=2,
            grid=(1,),
            in_specs=[
                pl.BlockSpec((rows, width), whole),
                pl.BlockSpec((1, rows, width), chunk),
                pl.BlockSpec((1, width), whole),
                store,
                store,
                pl.BlockSpec(memory_space=pltpu.VMEM),
                pl.BlockSpec(memory_space=pl.ANY),
            ],
            out_specs=[pl.BlockSpec((rows, width), whole), store],
            scratch_shapes=[pltpu.VMEM((rows, width), f32), pltpu.VMEM((rows, width), f32)],
        ),
        out_shape=[
            jax.ShapeDtypeStruct((rows, width), bf16),
            jax.ShapeDtypeStruct(gb.shape, gb.dtype),
        ],
        input_output_aliases={8: 1},
        compiler_params=params(),
        name="backward",
    )(t, s, recv, cots, gain, hb, db, masked, gb)


def ring(x, axis, distance):
    n = lax.axis_size(axis)
    return lax.ppermute(x, axis, [(i, (i + distance) % n) for i in range(n)])


def gather4(block, axis, direct):
    back = ring(block, axis, 1)
    ahead = ring(block, axis, -1)
    if direct:
        across = ring(block, axis, 2)
    else:
        half = block.shape[0] // 2
        across = jnp.concatenate([ring(back[:half], axis, 1), ring(ahead[half:], axis, -1)], axis=0)
    return jnp.stack([block, back, across, ahead])


def add(*terms):
    total = terms[0].astype(f32)
    for term in terms[1:]:
        total = total + term.astype(f32)
    return total


def scatter4(chunks, me, axis, dim):
    own, nxt, across, prev = [
        lax.dynamic_index_in_dim(chunks, lax.rem(me + k, 4), dim, keepdims=False) for k in range(4)
    ]
    return add(own, ring(nxt, axis, 1), ring(prev, axis, -1), ring(across, axis, 2))


def pairwise(x, axis, bit):
    n = lax.axis_size(axis)
    return x + lax.ppermute(x, axis, [(i, i ^ bit) for i in range(n)])


def token_product(x, g):
    return lax.dot_general(x, g, (((0,), (0,)), ((), ())), preferred_element_type=f32)


def body(activations, cotangent, weight, norm_gain, pair_mask, earlier_mask):
    section = lax.axis_index("section")
    y, x, core = (lax.axis_index(name) for name in DP)
    replica = (y * NX + x) * NC + core
    micro_count, row_count, width = activations.shape
    tokens = micro_count * row_count
    chunks = tokens // ROWS
    slots = chunks // STREAMS
    acts = activations.reshape(chunks, ROWS, width)
    cots = cotangent.reshape(chunks, ROWS, width)
    s = section.reshape(1).astype(jnp.int32)
    half = width // 2

    in_hbm = lambda array: pltpu.with_memory_space_constraint(array, pltpu.HBM)
    pairs = in_hbm(pair_mask[0])
    left, right, count, decay = prep(
        replica.reshape(1).astype(jnp.int32), in_hbm(weight[0]), pairs, in_hbm(earlier_mask[0])
    )

    left = gather4(left, "x", True)
    right = gather4(right, "y", True)
    rows = left.shape[1]
    right = gather4(right.reshape(4 * rows, half), "x", False).reshape(4, 4, rows, half)
    left = gather4(left.reshape(4 * rows, half), "y", False).reshape(4, 4, rows, half)
    right_other = ring(right, "core", 1)
    left_other = ring(left, "core", 1)
    pos = jnp.stack([y, x, core]).astype(jnp.int32)
    masked = expand(pos, left, right, left_other, right_other, pairs)

    fwd_ticks = slots + SECTIONS - 1
    zero = lambda dtype: jnp.zeros((chunks + 1, ROWS, width), dtype)
    buffers = (zero(bf16), zero(bf16), zero(f32))
    grads = zero(bf16)
    fwd = [acts[0] for _ in range(STREAMS)]
    bwd = [cots[0] for _ in range(STREAMS)]
    for tick in range(SECTIONS + fwd_ticks):
        now = jnp.full((1,), tick, jnp.int32)
        for k in range(STREAMS):
            if tick >= SECTIONS:
                out, grads = backward_step(
                    now, s, bwd[k], cots, norm_gain, masked, buffers, grads, slots, k * slots
                )
                if tick < SECTIONS + fwd_ticks - 1:
                    bwd[k] = ring(out, "section", -1)
            if tick < fwd_ticks:
                out, buffers = forward_step(
                    now, s, fwd[k], acts, norm_gain, masked, buffers, slots, k * slots
                )
                if tick < fwd_ticks - 1:
                    fwd[k] = ring(out, "section", 1)

    grads, core, y, x = lax.optimization_barrier((grads, core, y, x))
    normed = buffers[1][:chunks].reshape(tokens, width)
    grad = grads[:chunks].reshape(tokens, width)
    g_left, g_right = grad[:, :half], grad[:, half:]
    first = core == 0
    g_mine = jnp.where(first, g_left, g_right)
    normed_other = ring(normed, "core", 1)
    g_other = ring(jnp.where(first, g_right, g_left), "core", 1)
    quarter = half // 2
    parts = []
    for c in range(2):
        cols = slice(c * quarter, (c + 1) * quarter)
        partial = token_product(normed, g_mine[:, cols]) + token_product(normed_other, g_other[:, cols])
        parts.append(partial.astype(bf16).reshape(NY, NX, 2 * row_count, quarter))
    parts = lax.optimization_barrier(parts)
    part_l = scatter4(parts[0], x, "x", 1).astype(bf16)
    part_r = scatter4(parts[1], y, "y", 0).astype(bf16)
    part_l = scatter4(part_l, y, "y", 0)
    part_r = scatter4(part_r, x, "x", 0)
    mine = jnp.concatenate([part_l, part_r], axis=1)
    top, bottom = mine[:row_count], mine[row_count:]
    own = jnp.where(first, top, bottom)
    other = ring(jnp.where(first, bottom, top).astype(bf16), "core", 1).astype(f32)
    total = jnp.where(
        first, jnp.concatenate([own, other], axis=1), jnp.concatenate([other, own], axis=1)
    )
    gradient = total / math.sqrt(tokens * NY * NX * NC) + decay

    count = pairwise(pairwise(pairwise(count, "core", 1), "x", 1), "x", 2)
    count = pairwise(pairwise(count, "y", 1), "y", 2)
    return gradient[None], count[0, :1]


def solution(mesh):
    cube = Mesh(mesh.devices.reshape(NY, NX, NC, SECTIONS), (*DP, "section"))
    placed = (
        P(None, DP, None),
        P(None, DP, None),
        P("section", DP, None),
        P("section", None),
        P("section", None, None),
        P("section", DP, None),
    )
    return jax.shard_map(
        body,
        mesh=cube,
        in_specs=placed,
        out_specs=(P("section", DP, None), P("section")),
        check_vma=False,
    )
```
